128 devices in a mesh: dp: 1, tp: 2 (over core), cp: 64 (over z, y, x).
Axes of the slice: x: 4, y: 4, z: 4, core: 2. Of those that a mesh axis runs over, the one named last changes fastest.
Arguments:
- tokens_in: bfloat16 [16384, 3072], P(('dp', 'cp', 'tp'))
- grad_out: bfloat16 [16384, 3072], P(('dp', 'cp', 'tp'))
- w_query: bfloat16 [3072, 3072], P(None, 'tp')
- w_key: bfloat16 [3072, 1024], P(None, 'tp')
- w_value: bfloat16 [3072, 1024], P(None, 'tp')
- w_out: bfloat16 [3072, 3072], P('tp')
Outputs:
- output 1: bfloat16 [16384, 3072], P(('dp', 'cp', 'tp'))
- output 2: bfloat16 [16384, 3072], P(('dp', 'cp', 'tp'))
All inputs are finite; a program needn't handle non-finite values.
Results may differ from the reference program's by a relative error of at most 0.00949005.
Values are sent between devices in bfloat16 or wider.
A program may use at most 1 GiB of HBM per device.

```python
import math
import jax
import jax.numpy as jnp
from jax import lax

D = 3072
HQ = 24
HKV = 8
HEAD = 128
CP = 64
SEQ = 16384

GROUP_SIZE = HQ // HKV
SEQ_LOC = SEQ // CP
PIECE = SEQ_LOC // 2
ROW_BLOCK = 2 ** max(3, min(7, int(math.log2(max(1, 2 ** 22 // (SEQ * HQ))))))


def setup_inputs(seed: int = 0, part: int = 0) -> dict:
    base_key = jax.random.key(seed)
    data_key, weight_key = jax.random.split(base_key)
    part_key = jax.random.fold_in(data_key, part)
    key_x, key_dy = jax.random.split(part_key)
    key_q, key_k, key_v, key_o = jax.random.split(weight_key, 4)
    query_gain = math.sqrt(0.5 * math.log(SEQ))
    tokens_in = jax.random.normal(key_x, (SEQ, D), jnp.float32).astype(jnp.bfloat16)
    grad_out = jax.random.normal(key_dy, (SEQ, D), jnp.float32).astype(jnp.bfloat16)
    w_query = (jax.random.normal(key_q, (D, HQ * HEAD), jnp.float32) * (query_gain / math.sqrt(D))).astype(jnp.bfloat16)
    w_key = (jax.random.normal(key_k, (D, HKV * HEAD), jnp.float32) / math.sqrt(D)).astype(jnp.bfloat16)
    w_value = (jax.random.normal(key_v, (D, HKV * HEAD), jnp.float32) / math.sqrt(D)).astype(jnp.bfloat16)
    w_out = (jax.random.normal(key_o, (HQ * HEAD, D), jnp.float32) / math.sqrt(HQ * HEAD)).astype(jnp.bfloat16)
    return dict(tokens_in=tokens_in, grad_out=grad_out, w_query=w_query, w_key=w_key, w_value=w_value, w_out=w_out)


def fold_positions():
    row_ids = jnp.arange(SEQ, dtype=jnp.int32)
    shard_idx = row_ids // SEQ_LOC
    within = row_ids % SEQ_LOC
    piece_id = jnp.where(within < PIECE, shard_idx, 2 * CP - 1 - shard_idx)
    return piece_id * PIECE + within % PIECE


def reference(tokens_in, grad_out, w_query, w_key, w_value, w_out):
    score_scale = HEAD ** -0.5
    positions = fold_positions()
    queries = jnp.dot(tokens_in, w_query, preferred_element_type=jnp.float32).astype(jnp.bfloat16).reshape(SEQ, HKV, GROUP_SIZE, HEAD)
    keys_all = jnp.dot(tokens_in, w_key, preferred_element_type=jnp.float32).astype(jnp.bfloat16).reshape(SEQ, HKV, HEAD)
    values_all = jnp.dot(tokens_in, w_value, preferred_element_type=jnp.float32).astype(jnp.bfloat16).reshape(SEQ, HKV, HEAD)
    d_out = jnp.dot(grad_out, w_out.T, preferred_element_type=jnp.float32).astype(jnp.bfloat16).reshape(SEQ, HKV, GROUP_SIZE, HEAD)
    keys_f32 = keys_all.astype(jnp.float32)
    values_f32 = values_all.astype(jnp.float32)
    block_count = SEQ // ROW_BLOCK

    def block_step(acc_pair, blk_in):
        dk_acc, dv_acc = acc_pair
        q_blk, do_blk, pos_blk = blk_in
        query_f32 = q_blk.astype(jnp.float32)
        dout_f32 = do_blk.astype(jnp.float32)
        scores = jnp.einsum('qhgd,khd->hgqk', query_f32, keys_f32) * score_scale
        allowed = pos_blk[:, None] >= positions[None, :]
        scores = jnp.where(allowed, scores, -jnp.inf)
        log_norm = jax.nn.logsumexp(scores, axis=-1, keepdims=True)
        prob_f32 = jnp.exp(scores - log_norm).astype(jnp.bfloat16).astype(jnp.float32)
        out_blk = jnp.einsum('hgqk,khd->qhgd', prob_f32, values_f32).astype(jnp.bfloat16)
        row_delta = jnp.sum(dout_f32 * out_blk.astype(jnp.float32), axis=-1)
        d_prob = jnp.einsum('qhgd,khd->hgqk', dout_f32, values_f32)
        dscore_f32 = (prob_f32 * (d_prob - jnp.transpose(row_delta, (1, 2, 0))[..., None])).astype(jnp.bfloat16).astype(jnp.float32)
        dq_blk = (jnp.einsum('hgqk,khd->qhgd', dscore_f32, keys_f32) * score_scale).astype(jnp.bfloat16)
        dk_acc = dk_acc + jnp.einsum('hgqk,qhgd->khd', dscore_f32, query_f32) * score_scale
        dv_acc = dv_acc + jnp.einsum('hgqk,qhgd->khd', prob_f32, dout_f32)
        return (dk_acc, dv_acc), (out_blk, dq_blk)

    blk_inputs = (queries.reshape(block_count, ROW_BLOCK, HKV, GROUP_SIZE, HEAD), d_out.reshape(block_count, ROW_BLOCK, HKV, GROUP_SIZE, HEAD), positions.reshape(block_count, ROW_BLOCK))
    zeros_kv = jnp.zeros((SEQ, HKV, HEAD), jnp.float32)
    (dk_sum, dv_sum), (out_blocks, dq_blocks) = lax.scan(block_step, (zeros_kv, zeros_kv), blk_inputs)
    attn_out = out_blocks.reshape(SEQ, HQ * HEAD)
    d_query = dq_blocks.reshape(SEQ, HQ * HEAD)
    layer_out = jnp.dot(attn_out, w_out, preferred_element_type=jnp.float32).astype(jnp.bfloat16)
    grad_in = (jnp.dot(d_query, w_query.T, preferred_element_type=jnp.float32)
               + jnp.dot(dk_sum.astype(jnp.bfloat16).reshape(SEQ, HKV * HEAD), w_key.T, preferred_element_type=jnp.float32)
               + jnp.dot(dv_sum.astype(jnp.bfloat16).reshape(SEQ, HKV * HEAD), w_value.T, preferred_element_type=jnp.float32)).astype(jnp.bfloat16)
    return layer_out, grad_in
```

```python
import functools

import jax
import jax.numpy as jnp
from jax import lax
from jax.experimental import pallas as pl
from jax.experimental.pallas import tpu as pltpu
from jax.sharding import PartitionSpec as P

HD = 128
S = 16384
G = 3
KT = 512
UQ = 256
C2 = (HD ** -0.5) * 1.4426950408889634
TSC = HD ** -0.5
NEG = float(jnp.finfo(jnp.float32).min)
NINF = -float('inf')
BF = jnp.bfloat16
F32 = jnp.float32
MIB = 2 ** 20


def dg(a, b, ca, cb):
    return lax.dot_general(a, b, (((ca,), (cb,)), ((), ())), preferred_element_type=F32)


def split(c):
    z, y, x = c // 16, (c // 4) % 4, c % 4
    zz, yy = z // 2, y // 2
    xx = ((x + 1) // 2 + 1) % 2
    return (z + zz * (3 - 2 * z), y + yy * (3 - 2 * y), (x // 2 + yy) % 2), (zz, yy, xx)


def chip(grp, head):
    (za, ya, s), (zz, yy, xx) = grp, head
    z = za + zz * (3 - 2 * za)
    y = ya + yy * (3 - 2 * ya)
    hi = (s + yy) % 2
    return z * 16 + y * 4 + hi * (2 + xx) + (1 - hi) * (1 - xx)


def base_unit(grp, k):
    za, ya, s = grp
    return za * 8 + (ya + k * (3 - 2 * ya)) * 2 + s + k * (1 - 2 * s)


def unit_of(i, j):
    return (j // 2) * 32 + (j % 2) * 31 + (1 - 2 * (j % 2)) * i


def flip(grp, mask):
    return tuple(g + (1 - 2 * g) if (mask >> d) & 1 else g for d, g in enumerate(grp))


def quad_block(grp, k, zs, par):
    za, ya, s = grp
    ys = (zs + k) % 2
    z = za + zs * (3 - 2 * za)
    y = ya + ys * (3 - 2 * ya)
    return z * 16 + y * 4 + ((s + ys) % 2) * 2 + par


def dev(c, t):
    return {'tp': t, 'cp': c}


def me():
    c, t = lax.axis_index('cp'), lax.axis_index('tp')
    grp, head = split(c)
    return c, t, grp, head


def rd(start, n):
    return pl.ds(pl.multiple_of(start, n), n)


def greet(c, t, grp, head, cube):
    bar = pltpu.get_barrier_semaphore()
    n = 15
    for hh in range(8):
        for k in range(2):
            cc = chip(grp, (hh // 4, (hh // 2) % 2, hh % 2))

            @pl.when((cc != c) | (t != k))
            def _():
                pl.semaphore_signal(bar, 1, device_id=dev(cc, k), device_id_type=pl.DeviceIdType.MESH)
    if cube:
        for d in range(3):
            pl.semaphore_signal(bar, 1, device_id=dev(chip(flip(grp, 1 << d), head), t), device_id_type=pl.DeviceIdType.MESH)
        n += 3
    pl.semaphore_wait(bar, n)


def rcopy(src, dst, ssem, rsem, cc, k):
    return pltpu.make_async_remote_copy(src_ref=src, dst_ref=dst, send_sem=ssem, recv_sem=rsem, device_id=dev(cc, k), device_id_type=pl.DeviceIdType.MESH)


def send(src, dst, ssem, rsem, cc, k, own):
    @pl.when(own)
    def _():
        pltpu.make_async_copy(src, dst, rsem).start()

    @pl.when(jnp.logical_not(own))
    def _():
        rcopy(src, dst, ssem, rsem, cc, k).start()


def sent(src, dst, ssem, rsem, cc, k, own):
    @pl.when(jnp.logical_not(own))
    def _():
        rcopy(src, dst, ssem, rsem, cc, k).wait_send()


def got(dst, rsem):
    pltpu.make_async_copy(dst, dst, rsem).wait()


def order(it):
    return [(it + r) % 3 for r in range(3)]


def below(dims):
    masks = [0]
    for d in dims:
        masks += [m | (1 << d) for m in masks]
    return masks


VM = pl.BlockSpec(memory_space=pltpu.VMEM)
ANY = pl.BlockSpec(memory_space=pl.ANY)


def params(mib, cid=None):
    kw = {} if cid is None else dict(collective_id=cid, has_side_effects=True)
    return pltpu.CompilerParams(vmem_limit_bytes=mib * MIB, **kw)


def shape(s, d):
    return jax.ShapeDtypeStruct(s, d)


def pair_kernel(x_ref, dy_ref, xo_ref, do_ref, ssem, rsem):
    c, t = lax.axis_index('cp'), lax.axis_index('tp')
    bar = pltpu.get_barrier_semaphore()
    pl.semaphore_signal(bar, 1, device_id=dev(c, 1 - t), device_id_type=pl.DeviceIdType.MESH)
    pl.semaphore_wait(bar, 1)
    n = x_ref.shape[0]
    mine = rd(t * n, n)
    cps = [rcopy(src, dst.at[mine, :], ssem.at[e], rsem.at[e], c, 1 - t) for e, (src, dst) in enumerate(((x_ref, xo_ref), (dy_ref, do_ref)))]
    for cp in cps:
        cp.start()
    xo_ref[mine, :] = x_ref[...]
    do_ref[mine, :] = dy_ref[...]
    for cp in cps:
        cp.wait()


def pair_gather(x, dy):
    n, d = x.shape
    return pl.pallas_call(
        pair_kernel, out_shape=(shape((2 * n, d), x.dtype),) * 2, in_specs=[VM] * 2, out_specs=(VM,) * 2,
        scratch_shapes=[pltpu.SemaphoreType.DMA((2,)), pltpu.SemaphoreType.DMA((2,))],
        compiler_params=params(16, 0), name='pair_gather')(x, dy)


def pair_sum_kernel(y_ref, dx_ref, yo_ref, do_ref, ssem, rsem):
    c, t = lax.axis_index('cp'), lax.axis_index('tp')
    bar = pltpu.get_barrier_semaphore()
    pl.semaphore_signal(bar, 1, device_id=dev(c, 1 - t), device_id_type=pl.DeviceIdType.MESH)
    pl.semaphore_wait(bar, 1)
    n = yo_ref.shape[0]
    other = rd((1 - t) * n, n)
    cps = [rcopy(src.at[other, :], dst, ssem.at[e], rsem.at[e], c, 1 - t) for e, (src, dst) in enumerate(((y_ref, yo_ref), (dx_ref, do_ref)))]
    for cp in cps:
        cp.start()
    for cp in cps:
        cp.wait()


def pair_half(y, dx):
    n, d = y.shape
    return pl.pallas_call(
        pair_sum_kernel, out_shape=(shape((n // 2, d), y.dtype),) * 2, in_specs=[VM] * 2, out_specs=(VM,) * 2,
        scratch_shapes=[pltpu.SemaphoreType.DMA((2,)), pltpu.SemaphoreType.DMA((2,))],
        compiler_params=params(16, 1), name='pair_half')(y, dx)


def spread_kernel(q_ref, do_ref, k_ref, v_ref, qo_ref, doo_ref, ko_ref, vo_ref, ss1, rs1, ss2, rs2, ss3, rs3):
    c, t, grp, head = me()
    zb, yb, xb = head
    b = c
    par = c % 2
    k = (zb + yb) % 2
    greet(c, t, grp, head, True)

    def rows_q(zs, pr, e):
        j = zs + e * (3 - 2 * zs)
        return rd(j * UQ + (pr + e * (1 - 2 * pr)) * 128, 128)

    def rows_k(bb, e):
        return rd((bb + e * (127 - 2 * bb)) * 128, 128)

    def first(fn, kinds):
        for hh in range(4):
            cc = chip(grp, (t, hh // 2, hh % 2))
            own = (cc == c) & (k == t)
            for n in kinds:
                for e in range(2):
                    wide = HD if n < 2 else G * HD
                    src = (k_ref, v_ref, q_ref, do_ref)[n].at[e * 128:(e + 1) * 128, hh * wide:(hh + 1) * wide]
                    dst = (ko_ref, vo_ref, qo_ref, doo_ref)[n].at[rows_k(b, e) if n < 2 else rows_q(zb, par, e), :]
                    fn(src, dst, ss1.at[hh, n, e], rs1.at[zb * 2 + par, n, e], cc, k, own)

    def first_got(kinds):
        for zs in range(2):
            for pr in range(2):
                bb = quad_block(grp, t, zs, pr)
                for n in kinds:
                    for e in range(2):
                        dst = (ko_ref, vo_ref, qo_ref, doo_ref)[n].at[rows_k(bb, e) if n < 2 else rows_q(zs, pr, e), :]
                        got(dst, rs1.at[zs * 2 + pr, n, e])

    first(send, (0, 1))
    first(send, (2, 3))
    first_got((0, 1))

    def part(it, mask, kk):
        r = rd(unit_of(base_unit(flip(grp, mask), kk), it // 2) * UQ, UQ)
        return (ko_ref, vo_ref)[it % 2].at[r, :]

    def hop(it, r, mask):
        d = order(it)[r]
        ref = part(it, mask, t)
        m2 = mask | (1 << d)
        return rcopy(ref, ref, ss2.at[it, m2], rs2.at[it, m2], chip(flip(grp, 1 << d), head), t)

    def over(it, mask):
        ref = part(it, mask, t)
        return rcopy(ref, ref, ss3.at[it, mask], rs3.at[it, mask], c, 1 - t)

    for it in range(8):
        hop(it, 0, 0).start()
    for it in range(8):
        over(it, 0).start()
    for r in range(3):
        dims = [order(it)[:r] for it in range(8)]
        for it in range(8):
            new = [m | (1 << order(it)[r]) for m in below(dims[it])]
            for m in new:
                got(part(it, m, t), rs2.at[it, m])
            if r < 2:
                for m in below(order(it)[:r + 1]):
                    hop(it, r + 1, m).start()
            for m in new:
                over(it, m).start()
    first_got((2, 3))
    for it in range(8):
        for m in range(8):
            got(part(it, m, 1 - t), rs3.at[it, m])
    for it in range(8):
        for r in range(3):
            for m in below(order(it)[:r]):
                hop(it, r, m).wait_send()
        for m in range(8):
            over(it, m).wait_send()
    first(sent, (0, 1, 2, 3))


def spread(q, do, k, v):
    dma = pltpu.SemaphoreType.DMA
    return pl.pallas_call(
        spread_kernel,
        out_shape=(shape((4 * UQ, G * HD), BF),) * 2 + (shape((S, HD), BF),) * 2, in_specs=[VM] * 4, out_specs=(VM,) * 4,
        scratch_shapes=[dma((4, 4, 2)), dma((4, 4, 2)), dma((8, 8)), dma((8, 8)), dma((8, 8)), dma((8, 8))],
        compiler_params=params(32, 2), name='spread')(q, do, k, v)


def gather_back_kernel(o_ref, dq_ref, dk_ref, dv_ref, ob_ref, dqb_ref, dkb_ref, dvb_ref, buf, rb, fin, ss1, rs1, ss2, rs2, ss3, rs3):
    c, t, grp, head = me()
    zb, yb, xb = head
    kb = (zb + yb) % 2
    hm = yb * 2 + xb
    greet(c, t, grp, head, True)

    def rows(it, mask, kk):
        return rd(unit_of(base_unit(flip(grp, mask), kk), it // 2) * UQ, UQ)

    def over(it, mask):
        return rcopy((dk_ref, dv_ref)[it % 2].at[rows(it, mask, 1 - t), :], buf.at[it, mask], ss2.at[it, mask], rs2.at[it, mask], c, 1 - t)

    def back(fn, kinds):
        for j in range(4):
            zs = (0, 1, 1, 0)[j]
            for e in range(2):
                par = e if j < 2 else 1 - e
                half = 0 if j < 2 else 1
                cc = quad_block(grp, t, zs, par)
                own = (cc == c) & (zb == t)
                for n in kinds:
                    wide = G * HD if n < 2 else HD
                    if n < 2:
                        src = (o_ref, dq_ref)[n].at[j * UQ + e * 128:j * UQ + (e + 1) * 128, :]
                    else:
                        src = fin.at[j * 2 + n - 2, e * 128:(e + 1) * 128, :]
                    dst = (ob_ref, dqb_ref, dkb_ref, dvb_ref)[n].at[half * 128:(half + 1) * 128, pl.ds(pl.multiple_of(hm * wide, wide), wide)]
                    fn(src, dst, ss1.at[j, e, n], rs1.at[hm, half, n], cc, zb, own)

    def back_got(kinds):
        for hh in range(4):
            for half in range(2):
                for n in kinds:
                    wide = G * HD if n < 2 else HD
                    dst = (ob_ref, dqb_ref, dkb_ref, dvb_ref)[n].at[half * 128:(half + 1) * 128, hh * wide:(hh + 1) * wide]
                    got(dst, rs1.at[hh, half, n])

    def hop(it, r, mask):
        d = order(it)[r]
        m2 = mask ^ (1 << d)
        return rcopy(buf.at[it, mask], rb.at[it, mask], ss3.at[it, mask], rs3.at[it, mask], chip(flip(grp, 1 << d), head), t), m2

    for r in (2, 1, 0):
        for it in range(8):
            for m in below(order(it)[:r]):
                over(it, m | (1 << order(it)[r])).start()
    for it in range(8):
        over(it, 0).start()
    back(send, (0, 1))
    for r in (2, 1, 0):
        for it in range(8):
            for m in [m | (1 << order(it)[r]) for m in below(order(it)[:r])]:
                got(buf.at[it, m], rs2.at[it, m])
                tot = buf[it, m] + (dk_ref, dv_ref)[it % 2][rows(it, m, t), :]
                for r2 in range(2, r, -1):
                    m3 = m | (1 << order(it)[r2])
                    got(rb.at[it, m3], rs3.at[it, m3])
                    tot = tot + rb[it, m3]
                buf[it, m] = tot
                hop(it, r, m)[0].start()
    for it in range(8):
        got(buf.at[it, 0], rs2.at[it, 0])
        tot = buf[it, 0] + (dk_ref, dv_ref)[it % 2][rows(it, 0, t), :]
        for r2 in range(3):
            m3 = 1 << order(it)[r2]
            got(rb.at[it, m3], rs3.at[it, m3])
            tot = tot + rb[it, m3]
        fin[it] = tot.astype(BF)
    back(send, (2, 3))
    for it in range(8):
        for m in range(8):
            over(it, m).wait_send()
            if m:
                r = max(order(it).index(d) for d in range(3) if (m >> d) & 1)
                hop(it, r, m)[0].wait_send()
    back_got((0, 1, 2, 3))
    back(sent, (0, 1, 2, 3))


def gather_back(o, dq, dk, dv):
    dma = pltpu.SemaphoreType.DMA
    return pl.pallas_call(
        gather_back_kernel,
        out_shape=(shape((256, 4 * G * HD), BF),) * 2 + (shape((256, 4 * HD), BF),) * 2, in_specs=[VM] * 4, out_specs=(VM,) * 4,
        scratch_shapes=[pltpu.VMEM((8, 8, UQ, HD), F32), pltpu.VMEM((8, 8, UQ, HD), F32), pltpu.VMEM((8, UQ, HD), BF),
                        dma((4, 2, 4)), dma((4, 2, 4)), dma((8, 8)), dma((8, 8)), dma((8, 8)), dma((8, 8))],
        compiler_params=params(56, 3), name='gather_back')(o, dq, dk, dv)


def fwd_body(i, q_ref, k_ref, v_ref, o_ref, l2_ref, sa, sb, p_scr, m_scr, ot_scr):
    NT = S // KT
    diff = (lax.broadcasted_iota(jnp.int32, (KT, UQ), 0) - lax.broadcasted_iota(jnp.int32, (KT, UQ), 1))

    def one(idx, _):
        j, h = idx // G, idx % G
        u = unit_of(i, j)
        nt = (u + 2) // 2
        qh = q_ref[pl.ds(pl.multiple_of(j * UQ, UQ), UQ), pl.ds(pl.multiple_of(h * HD, HD), HD)]

        def score(t):
            return dg(k_ref[pl.ds(pl.multiple_of(t * KT, KT), KT), :], qh, 1, 1)

        def soft(s_ref, t, m, l, masked):
            s = s_ref[...] * C2
            if masked:
                s = jnp.where(diff <= u * UQ - t * KT, s, NINF)
            s3 = s.reshape(KT // 8, 8, UQ)
            mn = jnp.maximum(m, jnp.max(s3, axis=0))
            p3 = jnp.exp2(s3 - mn[None])
            l = l * jnp.exp2(m - mn) + jnp.sum(p3, axis=0)
            p_scr[pl.ds(pl.multiple_of(t * KT, KT), KT), :] = p3.reshape(KT, UQ)
            m_scr[t] = mn
            return mn, l

        sa[...] = score(0)
        m0 = jnp.full((8, UQ), NEG, F32)
        l0 = jnp.zeros((8, UQ), F32)
        nf = nt - 1

        def pair(tt, c):
            m, l = c
            t = tt * 2
            sb[...] = score(t + 1)
            m, l = soft(sa, t, m, l, False)
            sa[...] = score(t + 2)
            m, l = soft(sb, t + 1, m, l, False)
            return m, l
        m, l = lax.fori_loop(0, nf // 2, pair, (m0, l0))

        def odd(c):
            m, l = c
            sb[...] = score(nf)
            m, l = soft(sa, nf - 1, m, l, False)
            m, l = soft(sb, nf, m, l, True)
            return m, l

        def even(c):
            m, l = c
            return soft(sa, nf, m, l, True)
        m, l = lax.cond(nf % 2 == 1, odd, even, (m, l))
        mt = jnp.max(m, axis=0, keepdims=True)
        lt = jnp.sum(l * jnp.exp2(m - mt), axis=0, keepdims=True)
        l2 = mt + jnp.log2(lt)
        l2_ref[pl.ds(idx, 1), :] = l2

        @pl.when(nt < NT)
        def _():
            p_scr[pl.ds(pl.multiple_of(nt * KT, KT), KT), :] = jnp.zeros((KT, UQ), F32)
            m_scr[nt] = jnp.full((8, UQ), NEG, F32)
        ot_scr[...] = jnp.zeros_like(ot_scr)

        def pv(tt, _):
            acc = None
            for e in range(2):
                t = tt * 2 + e
                f = jnp.exp2(m_scr[t] - l2)
                p = p_scr[pl.ds(pl.multiple_of(t * KT, KT), KT), :].reshape(KT // 8, 8, UQ)
                pb = (p * f[None]).reshape(KT, UQ).astype(BF)
                r = dg(v_ref[pl.ds(pl.multiple_of(t * KT, KT), KT), :], pb, 0, 0)
                acc = r if acc is None else acc + r
            ot_scr[...] += acc
            return 0
        lax.fori_loop(0, (nt + 1) // 2, pv, 0)
        o_ref[pl.ds(pl.multiple_of(j * UQ, UQ), UQ), pl.ds(pl.multiple_of(h * HD, HD), HD)] = ot_scr[...].T.astype(BF)
        return 0
    lax.fori_loop(0, 4 * G, one, 0)


def bwd_body(i, q_ref, do_ref, o_ref, l2_ref, k_ref, v_ref, dq_ref, dk_ref, dv_ref, d_scr, dqt_scr, dka, dva):
    NT = S // KT
    diff = (lax.broadcasted_iota(jnp.int32, (KT, UQ), 0) - lax.broadcasted_iota(jnp.int32, (KT, UQ), 1))

    def prep(idx, _):
        j, h = idx // G, idx % G
        rows = pl.ds(pl.multiple_of(j * UQ, UQ), UQ)
        cols = pl.ds(pl.multiple_of(h * HD, HD), HD)
        prod = do_ref[rows, cols].astype(F32) * o_ref[rows, cols].astype(F32)
        d_scr[pl.ds(idx, 1), :] = jnp.sum(prod.T, axis=0, keepdims=True)
        dqt_scr[idx] = jnp.zeros((HD, UQ), F32)
        return 0
    lax.fori_loop(0, 4 * G, prep, 0)

    def tile(tt, _):
        t = NT - 1 - tt
        krows = pl.ds(pl.multiple_of(t * KT, KT), KT)
        dka[...] = jnp.zeros_like(dka)
        dva[...] = jnp.zeros_like(dva)

        def step(j, masked):
            u = unit_of(i, j)
            rows = pl.ds(pl.multiple_of(j * UQ, UQ), UQ)
            k = k_ref[krows, :]
            v = v_ref[krows, :]
            dv = None
            dk = None
            for h in range(G):
                idx = j * G + h
                cols = slice(h * HD, (h + 1) * HD)
                q = q_ref[rows, cols]
                do = do_ref[rows, cols]
                s = dg(k, q, 1, 1) * C2
                if masked:
                    s = jnp.where(diff <= u * UQ - t * KT, s, NINF)
                pb = jnp.exp2(s - l2_ref[pl.ds(idx, 1), :]).astype(BF)
                dp = dg(v, do, 1, 1)
                ds = (pb.astype(F32) * (dp - d_scr[pl.ds(idx, 1), :])).astype(BF)
                r1 = dg(pb, do, 1, 0)
                r2 = dg(ds, q, 1, 0)
                dv = r1 if dv is None else dv + r1
                dk = r2 if dk is None else dk + r2
                dqt_scr[idx] += dg(k, ds, 0, 0)
            dva[...] += dv
            dka[...] += dk

        for jj in range(4):
            j = 3 - jj
            u = unit_of(i, j)
            @pl.when(u // 2 > t)
            def _():
                step(j, False)

            @pl.when(u // 2 == t)
            def _():
                step(j, True)
        dk_ref[krows, :] = dka[...] * TSC
        dv_ref[krows, :] = dva[...]
        return 0
    lax.fori_loop(0, NT, tile, 0)

    def fin(idx, _):
        j, h = idx // G, idx % G
        rows = pl.ds(pl.multiple_of(j * UQ, UQ), UQ)
        cols = pl.ds(pl.multiple_of(h * HD, HD), HD)
        dq_ref[rows, cols] = (dqt_scr[idx] * TSC).T.astype(BF)
        return 0
    lax.fori_loop(0, 4 * G, fin, 0)


def fwd_kernel(*refs):
    _, t, grp, _ = me()
    fwd_body(base_unit(grp, t), *refs)


def bwd_kernel(*refs):
    _, t, grp, _ = me()
    bwd_body(base_unit(grp, t), *refs)


def attention_fwd(q, k, v):
    return pl.pallas_call(
        fwd_kernel, out_shape=(shape((4 * UQ, G * HD), BF), shape((4 * G, UQ), F32)), in_specs=[VM] * 3, out_specs=(VM, VM),
        scratch_shapes=[pltpu.VMEM((KT, UQ), F32), pltpu.VMEM((KT, UQ), F32), pltpu.VMEM((S, UQ), F32),
                        pltpu.VMEM((S // KT, 8, UQ), F32), pltpu.VMEM((HD, UQ), F32)],
        compiler_params=params(60), name='attention_fwd')(q, k, v)


def attention_bwd(q, do, o, l2, k, v):
    return pl.pallas_call(
        bwd_kernel, out_shape=(shape((4 * UQ, G * HD), BF), shape((S, HD), F32), shape((S, HD), F32)), in_specs=[VM] * 6, out_specs=(VM,) * 3,
        scratch_shapes=[pltpu.VMEM((4 * G, UQ), F32), pltpu.VMEM((4 * G, HD, UQ), F32), pltpu.VMEM((KT, HD), F32), pltpu.VMEM((KT, HD), F32)],
        compiler_params=params(60), name='attention_bwd')(q, do, o, l2, k, v)


def solution(mesh):
    row_spec = P(('dp', 'cp', 'tp'), None)

    def local_step(x_blk, dy_blk, w_query, w_key, w_value, w_out):
        x_loc, dy_loc = pair_gather(x_blk, dy_blk)
        keys = dg(x_loc, w_key, 1, 0).astype(BF)
        values = dg(x_loc, w_value, 1, 0).astype(BF)
        query = dg(x_loc, w_query, 1, 0).astype(BF)
        d_out = dg(dy_loc, w_out, 1, 1).astype(BF)
        q, do, k, v = spread(query, d_out, keys, values)
        o, l2 = attention_fwd(q, k, v)
        dq, dk, dv = attention_bwd(q, do, o, l2, k, v)
        ob, dqb, dkb, dvb = gather_back(o, dq, dk, dv)
        y_part = dg(ob, w_out, 1, 0)
        dx_part = dg(dqb, w_query, 1, 1) + dg(dkb, w_key, 1, 1) + dg(dvb, w_value, 1, 1)
        y_in, dx_in = pair_half(y_part, dx_part)
        n = y_in.shape[0]
        start = lax.axis_index('tp') * n
        y_own = lax.dynamic_slice_in_dim(y_part, start, n, 0)
        dx_own = lax.dynamic_slice_in_dim(dx_part, start, n, 0)
        return (y_own + y_in).astype(BF), (dx_own + dx_in).astype(BF)

    return jax.shard_map(local_step, mesh=mesh, in_specs=(row_spec, row_spec, P(None, 'tp'), P(None, 'tp'), P(None, 'tp'), P('tp', None)), out_specs=(row_spec, row_spec), check_vma=False)
```

```python
import functools

import jax
import jax.numpy as jnp
from jax import lax
from jax.experimental import pallas as pl
from jax.experimental.pallas import tpu as pltpu
from jax.sharding import PartitionSpec as P

HD = 128
S = 16384
G = 3
KT = 512
CH = 128
NG = 4
TG = KT * NG
UQ = 256
LAGS = (3, 7, 11, 15)
C2 = (HD ** -0.5) * 1.4426950408889634
TSC = HD ** -0.5
NEG = float(jnp.finfo(jnp.float32).min)
NINF = -float('inf')
BF = jnp.bfloat16
F32 = jnp.float32
MIB = 2 ** 20


def dg(a, b, ca, cb):
    return lax.dot_general(a, b, (((ca,), (cb,)), ((), ())), preferred_element_type=F32)


def split(c):
    z, y, x = c // 16, (c // 4) % 4, c % 4
    zz, yy = z // 2, y // 2
    xx = ((x + 1) // 2 + 1) % 2
    return (z + zz * (3 - 2 * z), y + yy * (3 - 2 * y), (x // 2 + yy) % 2), (zz, yy, xx)


def chip(grp, head):
    (za, ya, s), (zz, yy, xx) = grp, head
    z = za + zz * (3 - 2 * za)
    y = ya + yy * (3 - 2 * ya)
    hi = (s + yy) % 2
    return z * 16 + y * 4 + hi * (2 + xx) + (1 - hi) * (1 - xx)


def base_unit(grp, k):
    za, ya, s = grp
    return za * 8 + (ya + k * (3 - 2 * ya)) * 2 + s + k * (1 - 2 * s)


def unit_of(i, j):
    return (j // 2) * 32 + (j % 2) * 31 + (1 - 2 * (j % 2)) * i


def flip(grp, mask):
    return tuple(g + (1 - 2 * g) if (mask >> d) & 1 else g for d, g in enumerate(grp))


def quad_block(grp, k, zs, par):
    za, ya, s = grp
    ys = (zs + k) % 2
    z = za + zs * (3 - 2 * za)
    y = ya + ys * (3 - 2 * ya)
    return z * 16 + y * 4 + ((s + ys) % 2) * 2 + par


def dev(c, t):
    return {'tp': t, 'cp': c}


def me():
    c, t = lax.axis_index('cp'), lax.axis_index('tp')
    grp, head = split(c)
    return c, t, grp, head


def rd(start, n):
    return pl.ds(pl.multiple_of(start, n), n)


def greet(c, t, grp, head, cube):
    bar = pltpu.get_barrier_semaphore()
    n = 15
    for hh in range(8):
        for k in range(2):
            cc = chip(grp, (hh // 4, (hh // 2) % 2, hh % 2))

            @pl.when((cc != c) | (t != k))
            def _():
                pl.semaphore_signal(bar, 1, device_id=dev(cc, k), device_id_type=pl.DeviceIdType.MESH)
    if cube:
        for d in range(3):
            pl.semaphore_signal(bar, 1, device_id=dev(chip(flip(grp, 1 << d), head), t), device_id_type=pl.DeviceIdType.MESH)
        n += 3
    pl.semaphore_wait(bar, n)


def rcopy(src, dst, ssem, rsem, cc, k):
    return pltpu.make_async_remote_copy(src_ref=src, dst_ref=dst, send_sem=ssem, recv_sem=rsem, device_id=dev(cc, k), device_id_type=pl.DeviceIdType.MESH)


def send(src, dst, ssem, rsem, cc, k, own):
    @pl.when(own)
    def _():
        pltpu.make_async_copy(src, dst, rsem).start()

    @pl.when(jnp.logical_not(own))
    def _():
        rcopy(src, dst, ssem, rsem, cc, k).start()


def sent(src, dst, ssem, rsem, cc, k, own):
    @pl.when(jnp.logical_not(own))
    def _():
        rcopy(src, dst, ssem, rsem, cc, k).wait_send()


def got(dst, rsem):
    pltpu.make_async_copy(dst, dst, rsem).wait()


def order(it):
    return [(it + r) % 3 for r in range(3)]


def below(dims):
    masks = [0]
    for d in dims:
        masks += [m | (1 << d) for m in masks]
    return masks


VM = pl.BlockSpec(memory_space=pltpu.VMEM)
ANY = pl.BlockSpec(memory_space=pl.ANY)


def params(mib, cid=None):
    kw = {} if cid is None else dict(collective_id=cid, has_side_effects=True)
    return pltpu.CompilerParams(vmem_limit_bytes=mib * MIB, **kw)


def shape(s, d):
    return jax.ShapeDtypeStruct(s, d)


def pair_kernel(x_ref, dy_ref, xo_ref, do_ref, ssem, rsem):
    c, t = lax.axis_index('cp'), lax.axis_index('tp')
    bar = pltpu.get_barrier_semaphore()
    pl.semaphore_signal(bar, 1, device_id=dev(c, 1 - t), device_id_type=pl.DeviceIdType.MESH)
    pl.semaphore_wait(bar, 1)
    n = x_ref.shape[0]
    mine = rd(t * n, n)
    cps = [rcopy(src, dst.at[mine, :], ssem.at[e], rsem.at[e], c, 1 - t) for e, (src, dst) in enumerate(((x_ref, xo_ref), (dy_ref, do_ref)))]
    for cp in cps:
        cp.start()
    xo_ref[mine, :] = x_ref[...]
    do_ref[mine, :] = dy_ref[...]
    for cp in cps:
        cp.wait()


def pair_gather(x, dy):
    n, d = x.shape
    return pl.pallas_call(
        pair_kernel, out_shape=(shape((2 * n, d), x.dtype),) * 2, in_specs=[VM] * 2, out_specs=(VM,) * 2,
        scratch_shapes=[pltpu.SemaphoreType.DMA((2,)), pltpu.SemaphoreType.DMA((2,))],
        compiler_params=params(16, 0), name='pair_gather')(x, dy)


def pair_sum_kernel(y_ref, dx_ref, yo_ref, do_ref, ssem, rsem):
    c, t = lax.axis_index('cp'), lax.axis_index('tp')
    bar = pltpu.get_barrier_semaphore()
    pl.semaphore_signal(bar, 1, device_id=dev(c, 1 - t), device_id_type=pl.DeviceIdType.MESH)
    pl.semaphore_wait(bar, 1)
    n = yo_ref.shape[0]
    other = rd((1 - t) * n, n)
    cps = [rcopy(src.at[other, :], dst, ssem.at[e], rsem.at[e], c, 1 - t) for e, (src, dst) in enumerate(((y_ref, yo_ref), (dx_ref, do_ref)))]
    for cp in cps:
        cp.start()
    for cp in cps:
        cp.wait()


def pair_half(y, dx):
    n, d = y.shape
    return pl.pallas_call(
        pair_sum_kernel, out_shape=(shape((n // 2, d), y.dtype),) * 2, in_specs=[VM] * 2, out_specs=(VM,) * 2,
        scratch_shapes=[pltpu.SemaphoreType.DMA((2,)), pltpu.SemaphoreType.DMA((2,))],
        compiler_params=params(16, 1), name='pair_half')(y, dx)


def spread_kernel(q_ref, do_ref, k_ref, v_ref, qo_ref, doo_ref, ko_ref, vo_ref, ss1, rs1, ss2, rs2, ss3, rs3):
    c, t, grp, head = me()
    zb, yb, xb = head
    b = c
    par = c % 2
    k = (zb + yb) % 2
    greet(c, t, grp, head, True)

    def rows_q(zs, pr, e):
        j = zs + e * (3 - 2 * zs)
        return rd(j * UQ + (pr + e * (1 - 2 * pr)) * 128, 128)

    def rows_k(bb, e):
        return rd((bb + e * (127 - 2 * bb)) * 128, 128)

    def first(fn, kinds):
        for hh in range(4):
            cc = chip(grp, (t, hh // 2, hh % 2))
            own = (cc == c) & (k == t)
            for n in kinds:
                for e in range(2):
                    wide = HD if n < 2 else G * HD
                    src = (k_ref, v_ref, q_ref, do_ref)[n].at[e * 128:(e + 1) * 128, hh * wide:(hh + 1) * wide]
                    dst = (ko_ref, vo_ref, qo_ref, doo_ref)[n].at[rows_k(b, e) if n < 2 else rows_q(zb, par, e), :]
                    fn(src, dst, ss1.at[hh, n, e], rs1.at[zb * 2 + par, n, e], cc, k, own)

    def first_got(kinds):
        for zs in range(2):
            for pr in range(2):
                bb = quad_block(grp, t, zs, pr)
                for n in kinds:
                    for e in range(2):
                        dst = (ko_ref, vo_ref, qo_ref, doo_ref)[n].at[rows_k(bb, e) if n < 2 else rows_q(zs, pr, e), :]
                        got(dst, rs1.at[zs * 2 + pr, n, e])

    first(send, (0, 1))
    first(send, (2, 3))
    first_got((0, 1))

    def part(it, mask, kk):
        r = rd(unit_of(base_unit(flip(grp, mask), kk), it // 2) * UQ, UQ)
        return (ko_ref, vo_ref)[it % 2].at[r, :]

    def hop(it, r, mask):
        d = order(it)[r]
        ref = part(it, mask, t)
        m2 = mask | (1 << d)
        return rcopy(ref, ref, ss2.at[it, m2], rs2.at[it, m2], chip(flip(grp, 1 << d), head), t)

    def over(it, mask):
        ref = part(it, mask, t)
        return rcopy(ref, ref, ss3.at[it, mask], rs3.at[it, mask], c, 1 - t)

    for it in range(8):
        hop(it, 0, 0).start()
    for it in range(8):
        over(it, 0).start()
    for r in range(3):
        dims = [order(it)[:r] for it in range(8)]
        for it in range(8):
            new = [m | (1 << order(it)[r]) for m in below(dims[it])]
            for m in new:
                got(part(it, m, t), rs2.at[it, m])
            if r < 2:
                for m in below(order(it)[:r + 1]):
                    hop(it, r + 1, m).start()
            for m in new:
                over(it, m).start()
    first_got((2, 3))
    for it in range(8):
        for m in range(8):
            got(part(it, m, 1 - t), rs3.at[it, m])
    for it in range(8):
        for r in range(3):
            for m in below(order(it)[:r]):
                hop(it, r, m).wait_send()
        for m in range(8):
            over(it, m).wait_send()
    first(sent, (0, 1, 2, 3))


def spread(q, do, k, v):
    dma = pltpu.SemaphoreType.DMA
    return pl.pallas_call(
        spread_kernel,
        out_shape=(shape((4 * UQ, G * HD), BF),) * 2 + (shape((S, HD), BF),) * 2, in_specs=[VM] * 4, out_specs=(VM,) * 4,
        scratch_shapes=[dma((4, 4, 2)), dma((4, 4, 2)), dma((8, 8)), dma((8, 8)), dma((8, 8)), dma((8, 8))],
        compiler_params=params(32, 2), name='spread')(q, do, k, v)


def transpose_into(x_ref, xt_ref, n):
    def body(t, _):
        r = pl.ds(pl.multiple_of(t * KT, KT), KT)
        xt_ref[:, r] = x_ref[r, :].T
        return 0
    lax.fori_loop(0, n // KT, body, 0)


def rows_of(j):
    return pl.ds(pl.multiple_of(j * UQ, UQ), UQ)


def cols_of(h):
    return pl.ds(pl.multiple_of(h * HD, HD), HD)


def fwd_body(i, q_ref, k_ref, v_ref, o_ref, l2_ref, sa, sb, p_scr, m_scr, ot_scr, vt_scr, qt_scr):
    diff = (lax.broadcasted_iota(jnp.int32, (CH, UQ), 0) - lax.broadcasted_iota(jnp.int32, (CH, UQ), 1))
    transpose_into(v_ref, vt_scr, S)
    NC = KT // CH

    def one(idx, _):
        j, h = idx // G, idx % G
        u = unit_of(i, j)
        ng = (u * UQ) // TG + 1
        qt_scr[...] = q_ref[rows_of(j), cols_of(h)].T

        def score(t):
            return dg(k_ref[pl.ds(pl.multiple_of(t * KT, KT), KT), :], qt_scr[...], 1, 0)

        def soft(s_ref, t, m, l, masked):
            for c in range(NC):
                s = s_ref[c * CH:(c + 1) * CH, :] * C2
                if masked:
                    s = jnp.where(diff <= u * UQ - t * KT - c * CH, s, NINF)
                s3 = s.reshape(CH // 8, 8, UQ)
                mn = jnp.maximum(m, jnp.max(s3, axis=0))
                p3 = jnp.exp2(s3 - mn[None])
                l = l * jnp.exp2(m - mn) + jnp.sum(p3, axis=0)
                m = mn
                p_scr[pl.ds(pl.multiple_of(t * KT + c * CH, CH), CH), :] = p3.reshape(CH, UQ)
                m_scr[t * NC + c] = mn
            return m, l

        sa[...] = score(0)
        m0 = jnp.full((8, UQ), NEG, F32)
        l0 = jnp.zeros((8, UQ), F32)

        def group(g, c, masked):
            m, l = c
            t = g * NG
            for e in range(1, NG):
                sb[e - 1] = score(t + e)
            m, l = soft(sa, t, m, l, masked)
            if not masked:
                sa[...] = score(t + NG)
            for e in range(1, NG):
                m, l = soft(sb.at[e - 1], t + e, m, l, masked)
            return m, l
        m, l = lax.fori_loop(0, ng - 1, lambda g, c: group(g, c, False), (m0, l0))
        m, l = group(ng - 1, (m, l), True)
        mt = jnp.max(m, axis=0, keepdims=True)
        lt = jnp.sum(l * jnp.exp2(m - mt), axis=0, keepdims=True)
        l2 = mt + jnp.log2(lt)
        l2_ref[pl.ds(idx, 1), :] = l2
        ot_scr[...] = jnp.zeros_like(ot_scr)

        def pv(g, _):
            acc = None
            for e in range(NG):
                t = g * NG + e
                ps = []
                for c in range(NC):
                    f = jnp.exp2(m_scr[t * NC + c] - l2)
                    p = p_scr[pl.ds(pl.multiple_of(t * KT + c * CH, CH), CH), :].reshape(CH // 8, 8, UQ)
                    ps.append((p * f[None]).reshape(CH, UQ).astype(BF))
                r = dg(vt_scr[:, pl.ds(pl.multiple_of(t * KT, KT), KT)], jnp.concatenate(ps, 0), 1, 0)
                acc = r if acc is None else acc + r
            ot_scr[...] += acc
            return 0
        lax.fori_loop(0, ng, pv, 0)
        o_ref[rows_of(j), cols_of(h)] = ot_scr[...].T.astype(BF)
        return 0
    lax.fori_loop(0, 4 * G, one, 0)


def owners(t):
    j = t // 8
    odd, hi = j % 2, j // 2
    h = (1 - 2 * odd) * t + odd * (15 + 16 * hi) - (1 - odd) * 16 * hi
    za, yk = h // 4, h % 4
    k = yk // 2
    return j, k, za, yk + k * (3 - 2 * yk), (odd + k) % 2


def bwd_kernel(q_ref, do_ref, o_ref, l2_ref, k_ref, v_ref, ob_ref, dqb_ref, dkb_ref, dvb_ref,
               dq_ref, dkv, d_scr, dqt_scr, qt_scr, dot_scr, s_scr, dp_scr,
               rb0, rb1, rb2, rb3, fin, ssb, rsb, ss0, rs0, ss1, rs1, ss2, rs2, ss3, rs3):
    c, t_me, grp, head = me()
    zb, yb, xb = head
    hm = yb * 2 + xb
    i = base_unit(grp, t_me)
    NT = S // KT
    nbrs = [chip(flip(grp, 1 << d), head) for d in range(3)]

    def back(fn, j, n):
        zs = ((j + 1) // 2) % 2
        half = j // 2
        for e in range(2):
            par = e + half * (1 - 2 * e)
            cc = quad_block(grp, t_me, zs, par)
            own = (cc == c) & (zb == t_me)
            wide = G * HD if n < 2 else HD
            if n < 2:
                src = (o_ref, dq_ref)[n].at[rd(j * UQ + e * 128, 128), :]
            else:
                src = fin.at[j, n - 2, e * 128:(e + 1) * 128, :]
            dst = (ob_ref, dqb_ref, dkb_ref, dvb_ref)[n].at[rd(half * 128, 128), pl.ds(pl.multiple_of(hm * wide, wide), wide)]
            fn(src, dst, ssb.at[j, e, n], rsb.at[hm, half, n], cc, zb, own)

    def back_got(n):
        wide = G * HD if n < 2 else HD
        for hh in range(4):
            for half in range(2):
                got((ob_ref, dqb_ref, dkb_ref, dvb_ref)[n].at[half * 128:(half + 1) * 128, hh * wide:(hh + 1) * wide], rsb.at[hh, half, n])

    def item(n, e):
        t = tile_at(n)
        j, k, za, ya, s0 = owners(t)
        hi = j // 2
        same = [za == grp[0], ya == grp[1], (s0 + e) % 2 == grp[2]]
        if e:
            same = same[::-1]
            slots = [(j * 2 + 1) * 4 + za * 2 + ya, hi * 4 + za * 2 + ya, hi * 2 + za, hi]
        else:
            slots = [j * 8 + za * 2 + ya, j * 2 + ya, j, hi]
        there = [k == t_me]
        for d in range(3):
            there.append(there[d] & same[d])
        sends = [k != t_me] + [there[d] & jnp.logical_not(same[d]) for d in range(3)]
        return 2 * t + e, j, slots, there, sends

    def link(n, e, u, slots, r):
        if r == 0:
            return rcopy(dkv.at[u], rb0.at[slots[0]], ss0.at[slots[0]], rs0.at[slots[0]], c, 1 - t_me)
        rb, ss, rs = ((rb1, ss1, rs1), (rb2, ss2, rs2), (rb3, ss3, rs3))[r - 1]
        return rcopy(rb0.at[slots[0]], rb.at[e, slots[r]], ss.at[e, slots[r]], rs.at[e, slots[r]], nbrs[3 - r if e else r - 1], t_me)

    def over(n):
        for e in range(2):
            u, _, slots, _, sends = item(n, e)

            @pl.when(sends[0])
            def _():
                link(n, e, u, slots, 0).start()

    def stage(n, r):
        for e in range(2):
            u, j, slots, there, sends = item(n, e)
            acc = rb0.at[slots[0]]

            @pl.when(there[r])
            def _():
                if r == 0:
                    got(acc, rs0.at[slots[0]])
                    acc[...] = acc[...] + dkv[u]
                else:
                    rb, rs = ((rb1, rs1), (rb2, rs2), (rb3, rs3))[r - 1]
                    new = rb.at[e, slots[r]]
                    got(new, rs.at[e, slots[r]])
                    if r < 3:
                        acc[...] = acc[...] + new[...]
                    else:
                        fin[j, 0] = ((acc[0] + new[0]) * TSC).astype(BF)
                        fin[j, 1] = (acc[1] + new[1]).astype(BF)
                        back(send, j, 2)
                        back(send, j, 3)
            if r < 3:
                @pl.when(sends[r + 1])
                def _():
                    link(n, e, u, slots, r + 1).start()

    def tile_at(n):
        n = jnp.minimum(n, NT - 1)
        b, a, w = n // 8, (n // 2) % 4, n % 2
        low = 4 * (b + 1 - 2 * (b % 2)) + a + 2 - 4 * (a // 2)
        return (1 - w) * (31 - 4 * b - a) + w * low

    def sums(n):
        for r in range(4):
            m = n - LAGS[r]

            @pl.when((m >= 0) & (m < NT))
            def _():
                stage(m, r)

    greet(c, t_me, grp, head, True)
    for j in range(4):
        back(send, j, 0)

    diff = (lax.broadcasted_iota(jnp.int32, (KT, UQ), 0) - lax.broadcasted_iota(jnp.int32, (KT, UQ), 1))

    def prep(idx, _):
        j, h = idx // G, idx % G
        rows, cols = rows_of(j), cols_of(h)
        prod = do_ref[rows, cols].astype(F32) * o_ref[rows, cols].astype(F32)
        d_scr[pl.ds(idx, 1), :] = jnp.sum(prod.T, axis=0, keepdims=True)
        dqt_scr[idx] = jnp.zeros((HD, UQ), F32)
        qt_scr[idx] = q_ref[rows, cols].T
        dot_scr[idx] = do_ref[rows, cols].T
        return 0
    lax.fori_loop(0, 4 * G, prep, 0)
    last = [unit_of(i, j) // 2 for j in range(4)]

    def keys(t):
        return rd(t * KT, KT)

    def dots(t, j, h):
        s_scr[h] = dg(k_ref[keys(t), :], qt_scr[j * G + h], 1, 0)
        dp_scr[h] = dg(v_ref[keys(t), :], dot_scr[j * G + h], 1, 0)

    def first(n):
        return tile_at(n + (last[3] < tile_at(n)).astype(jnp.int32))

    for h in range(G):
        dots(first(jnp.int32(0)), 3, h)

    def tile(n, _):
        t = tile_at(n)
        krows = keys(t)
        units = 0
        for j in range(4):
            units = units + (last[j] >= t).astype(jnp.int32)
        pair = pl.ds(2 * t, 2)
        dkv[pair] = jnp.zeros((2, 2, UQ, HD), F32)

        def step(jj, _):
            j = 3 - jj
            wrap = jj + 1 == units
            tn = jnp.where(wrap, first(n + 1), t)
            jn = jnp.where(wrap, 3, j - 1)
            off = unit_of(i, j) * UQ - t * KT
            rows = rows_of(j)
            k = k_ref[krows, :]
            dv = None
            dk = None
            for h in range(G):
                idx = j * G + h
                cols = slice(h * HD, (h + 1) * HD)
                q = q_ref[rows, cols]
                do = do_ref[rows, cols]
                s = jnp.where(diff <= off, s_scr[h] * C2, NINF)
                pb = jnp.exp2(s - l2_ref[pl.ds(idx, 1), :]).astype(BF)
                ds = (pb.astype(F32) * (dp_scr[h] - d_scr[pl.ds(idx, 1), :])).astype(BF)
                dots(tn, jn, h)
                r1 = dg(pb, do, 1, 0)
                r2 = dg(ds, q, 1, 0)
                dv = r1 if dv is None else dv + r1
                dk = r2 if dk is None else dk + r2
                dqt_scr[idx] += dg(k, ds, 0, 0)
            dkv[pair, 0] += dk.reshape(2, UQ, HD)
            dkv[pair, 1] += dv.reshape(2, UQ, HD)
            return 0
        lax.fori_loop(0, units, step, 0)
        over(n)
        sums(n)
        return 0
    lax.fori_loop(0, NT, tile, 0)

    def final(idx, _):
        j, h = idx // G, idx % G
        dq_ref[rows_of(j), cols_of(h)] = (dqt_scr[idx] * TSC).T.astype(BF)
        return 0
    lax.fori_loop(0, 4 * G, final, 0)
    for j in range(4):
        back(send, j, 1)

    def drain(n, _):
        sums(n)
        return 0
    lax.fori_loop(NT, NT + LAGS[3], drain, 0)

    def close(n, _):
        for e in range(2):
            u, _, slots, _, sends = item(n, e)
            for r in range(4):
                @pl.when(sends[r])
                def _():
                    link(n, e, u, slots, r).wait_send()
        return 0
    lax.fori_loop(0, NT, close, 0)
    for n in range(4):
        back_got(n)
        for j in range(4):
            back(sent, j, n)


def attention_bwd(q, do, o, l2, k, v):
    dma = pltpu.SemaphoreType.DMA
    vm = pltpu.VMEM
    sems = [dma((4, 2, 4)), dma((4, 2, 4))]
    for n in ((32,), (2, 8), (2, 4), (2, 2)):
        sems += [dma(n), dma(n)]
    return pl.pallas_call(
        bwd_kernel,
        out_shape=(shape((256, 4 * G * HD), BF),) * 2 + (shape((256, 4 * HD), BF),) * 2, in_specs=[VM] * 6, out_specs=(VM,) * 4,
        scratch_shapes=[vm((4 * UQ, G * HD), BF), vm((S // UQ, 2, UQ, HD), F32), vm((4 * G, UQ), F32), vm((4 * G, HD, UQ), F32),
                        vm((4 * G, HD, UQ), BF), vm((4 * G, HD, UQ), BF), vm((G, KT, UQ), F32), vm((G, KT, UQ), F32),
                        vm((32, 2, UQ, HD), F32), vm((2, 8, 2, UQ, HD), F32), vm((2, 4, 2, UQ, HD), F32), vm((2, 2, 2, UQ, HD), F32), vm((4, 2, UQ, HD), BF)] + sems,
        compiler_params=params(62, 3), name='attention_bwd')(q, do, o, l2, k, v)


def fwd_kernel(*refs):
    _, t, grp, _ = me()
    fwd_body(base_unit(grp, t), *refs)


def attention_fwd(q, k, v):
    return pl.pallas_call(
        fwd_kernel, out_shape=(shape((4 * UQ, G * HD), BF), shape((4 * G, UQ), F32)), in_specs=[VM] * 3, out_specs=(VM, VM),
        scratch_shapes=[pltpu.VMEM((KT, UQ), F32), pltpu.VMEM((NG - 1, KT, UQ), F32), pltpu.VMEM((S, UQ), F32),
            pltpu.VMEM((S // CH, 8, UQ), F32), pltpu.VMEM((HD, UQ), F32), pltpu.VMEM((HD, S), BF), pltpu.VMEM((HD, UQ), BF)],
        compiler_params=params(60), name='attention_fwd')(q, k, v)


def solution(mesh):
    row_spec = P(('dp', 'cp', 'tp'), None)

    def local_step(x_blk, dy_blk, w_query, w_key, w_value, w_out):
        x_loc, dy_loc = pair_gather(x_blk, dy_blk)
        keys = dg(x_loc, w_key, 1, 0).astype(BF)
        values = dg(x_loc, w_value, 1, 0).astype(BF)
        query = dg(x_loc, w_query, 1, 0).astype(BF)
        d_out = dg(dy_loc, w_out, 1, 1).astype(BF)
        q, do, k, v = spread(query, d_out, keys, values)
        o, l2 = attention_fwd(q, k, v)
        ob, dqb, dkb, dvb = attention_bwd(q, do, o, l2, k, v)
        y_part = dg(ob, w_out, 1, 0)
        dx_part = dg(dqb, w_query, 1, 1) + dg(dkb, w_key, 1, 1) + dg(dvb, w_value, 1, 1)
        y_in, dx_in = pair_half(y_part, dx_part)
        n = y_in.shape[0]
        start = lax.axis_index('tp') * n
        y_own = lax.dynamic_slice_in_dim(y_part, start, n, 0)
        dx_own = lax.dynamic_slice_in_dim(dx_part, start, n, 0)
        return (y_own + y_in).astype(BF), (dx_own + dx_in).astype(BF)

    return jax.shard_map(local_step, mesh=mesh, in_specs=(row_spec, row_spec, P(None, 'tp'), P(None, 'tp'), P(None, 'tp'), P('tp', None)), out_specs=(row_spec, row_spec), check_vma=False)
```

```python
import functools

import jax
import jax.numpy as jnp
from jax import lax
from jax.experimental import pallas as pl
from jax.experimental.pallas import tpu as pltpu
from jax.sharding import PartitionSpec as P

HD = 128
PC = HD
S = 16384
G = 3
KT = 512
NG = 4
TG = KT * NG
UQ = 256
LAGS = (3, 7, 11, 15)
TSC = HD ** -0.5
C2 = TSC * 1.4426950408889634
NINF = -float('inf')
BF = jnp.bfloat16
F32 = jnp.float32


def dg(a, b, ca, cb):
    return lax.dot_general(a, b, (((ca,), (cb,)), ((), ())), preferred_element_type=F32)


def each(n, first=0):
    def run(body):
        def step(m, _):
            body(m)
            return 0
        lax.fori_loop(first, n, step, 0)
    return run


def mm(a, b):
    return dg(a, b, 1, 0)


def mt(a, b):
    return dg(a, b, 1, 1)


def tm(a, b):
    return dg(a, b, 0, 0)


def mirror(v, h):
    return v + h * (3 - 2 * v)


def turn(v, e):
    return v + e * (1 - 2 * v)


def split(c):
    co = (c // 16, (c // 4) % 4, c % 4)
    return tuple(mirror(v, v // 2) for v in co), tuple(v // 2 for v in co)


def chip(grp, head):
    z, y, x = (mirror(g, h) for g, h in zip(grp, head))
    return z * 16 + y * 4 + x


def base_tile(grp, k):
    return grp[0] * 4 + mirror(grp[1], k)


def tile_of(i, j):
    odd = j & 1
    return (j >> 1) * 16 + odd * 15 + (1 - 2 * odd) * i


def ahead(xa):
    row = lax.broadcasted_iota(jnp.int32, (KT, UQ), 0)
    col = lax.broadcasted_iota(jnp.int32, (KT, UQ), 1)
    quarter = row // PC
    piece = jnp.where(quarter == 0, 0, jnp.where(quarter == 1, 3, quarter - 1))
    late = col // PC
    return (piece - mirror(xa, late)) * PC + row % PC - col % PC


def flip(grp, mask):
    return tuple(1 - g if (mask >> d) & 1 else g for d, g in enumerate(grp))


def quad_block(grp, k, zs, par):
    return chip(grp, (zs, (zs + k) % 2, par))


def dev(c, t):
    return {'tp': t, 'cp': c}


def me():
    c, t = lax.axis_index('cp'), lax.axis_index('tp')
    grp, head = split(c)
    return c, t, grp, head


def line(n):
    return pl.ds(n, 1)


def rd(start, n):
    return pl.ds(pl.multiple_of(start, n), n)


def greet(c, t, grp, head):
    bar = pltpu.get_barrier_semaphore()
    for hh in range(8):
        for k in range(2):
            cc = chip(grp, (hh // 4, (hh // 2) % 2, hh % 2))

            @pl.when((cc != c) | (t != k))
            def _():
                pl.semaphore_signal(bar, 1, device_id=dev(cc, k), device_id_type=pl.DeviceIdType.MESH)
    for d in range(3):
        pl.semaphore_signal(bar, 1, device_id=dev(chip(flip(grp, 1 << d), head), t), device_id_type=pl.DeviceIdType.MESH)
    pl.semaphore_wait(bar, 18)


def rcopy(src, dst, ssem, rsem, cc, k):
    return pltpu.make_async_remote_copy(src_ref=src, dst_ref=dst, send_sem=ssem, recv_sem=rsem, device_id=dev(cc, k), device_id_type=pl.DeviceIdType.MESH)


def send(src, dst, ssem, rsem, cc, k, own):
    @pl.when(own)
    def _():
        pltpu.make_async_copy(src, dst, rsem).start()

    @pl.when(jnp.logical_not(own))
    def _():
        rcopy(src, dst, ssem, rsem, cc, k).start()


def sent(src, dst, ssem, rsem, cc, k, own):
    @pl.when(jnp.logical_not(own))
    def _():
        rcopy(src, dst, ssem, rsem, cc, k).wait_send()


def got(dst, rsem):
    pltpu.make_async_copy(dst, dst, rsem).wait()


def order(it):
    return [(it + r) % 3 for r in range(3)]


def below(dims):
    masks = [0]
    for d in dims:
        masks += [m | (1 << d) for m in masks]
    return masks


VM = pl.BlockSpec(memory_space=pltpu.VMEM)
ANY = pl.BlockSpec(memory_space=pl.ANY)
HB = pl.BlockSpec(memory_space=pltpu.HBM)


def params(kib, cid):
    return pltpu.CompilerParams(vmem_limit_bytes=kib * 1024, collective_id=cid, has_side_effects=True)


def shape(s, d):
    return jax.ShapeDtypeStruct(s, d)


def rows_of(j):
    return rd(j * UQ, UQ)


def cols_of(h):
    return rd(h * HD, HD)


PB = UQ


def forward(x_ref, dy_ref, wq, wk, wv, wo, qo_ref, doo_ref, ko_ref, vo_ref, o_ref, l2_ref, qt_scr, s_scr, ot_scr,
            kvq, dout, xp, dyp, wa, wb, m_scr, l_scr, mx_scr, xss, xrs, lsem, ss1, rs1, ss2, rs2, ss3, rs3):
    c, t, grp, head = me()
    zb, yb, xb = head
    par = xb
    k = (zb + yb) % 2
    i = base_tile(grp, t)
    outs = (ko_ref, vo_ref, qo_ref, doo_ref)
    half = x_ref.shape[0]
    kv_blocks, q_blocks = 2 * wk.shape[1] // PB, wq.shape[1] // PB

    def start(cp):
        cp.start()

    def wait(cp):
        cp.wait()

    def load(b, fn):
        for w, at, n in ((wk, 0, kv_blocks // 2), (wv, kv_blocks // 2, kv_blocks // 2), (wq, kv_blocks, q_blocks)):
            @pl.when((b >= at) & (b < at + n))
            def _():
                fn(pltpu.make_async_copy(w.at[:, rd((b - at) * PB, PB)], wa.at[b & 1], lsem.at[0, b & 1]))

    def load_out(b, fn):
        fn(pltpu.make_async_copy(wo.at[rd(b * PB, PB), :], wb.at[b & 1], lsem.at[1, b & 1]))

    def put(ref, b, r):
        ref[rd(t * half, half), rd(b * PB, PB)] = r[:half].astype(BF)
        ref[rd((1 - t) * half, half), rd(b * PB, PB)] = r[half:].astype(BF)

    def project(b):
        pltpu.make_async_copy(wa.at[b & 1], wa.at[b & 1], lsem.at[0, b & 1]).wait()
        put(kvq, b, mm(jnp.concatenate([x_ref[...], xp[...]], 0), wa[b & 1]))
        load(b + 2, start)

    def project_out(b):
        load_out(b, wait)
        put(dout, b, mt(jnp.concatenate([dy_ref[...], dyp[...]], 0), wb[b & 1]))

        @pl.when(b + 2 < q_blocks)
        def _():
            load_out(b + 2, start)

    for b in range(2):
        load(jnp.int32(b), start)
        load_out(b, start)
    greet(c, t, grp, head)
    swaps = [rcopy(src, dst, xss.at[n], xrs.at[n], c, 1 - t) for n, (src, dst) in enumerate(((x_ref, xp), (dy_ref, dyp)))]
    for cp in swaps:
        cp.start()

    def rows_q(zs, pr, e):
        return rd(mirror(zs, e) * UQ + turn(pr, e) * PC, PC)

    def rows_k(bb, e):
        q, half = bb // 4, (bb % 4) // 2
        return rd((q + e * (31 - 2 * q)) * KT + grp[2] * UQ + turn(half, e) * PC, PC)

    def first(fn, kinds, halves=(0, 1)):
        for e in halves:
            for hh in range(4):
                cc = chip(grp, (t, hh // 2, hh % 2))
                own = (cc == c) & (k == t)
                for n in kinds:
                    wide = HD if n < 2 else G * HD
                    at = (0, kv_blocks // 2 * PB, kv_blocks * PB, 0)[n] + hh * wide
                    src = (kvq, kvq, kvq, dout)[n].at[e * PC:(e + 1) * PC, at:at + wide]
                    dst = outs[n].at[rows_k(c, e) if n < 2 else rows_q(zb, par, e), :]
                    fn(src, dst, ss1.at[hh, n, e], rs1.at[zb * 2 + par, n, e], cc, k, own)

    def first_got(kinds, halves=(0, 1)):
        for zs in range(2):
            for pr in range(2):
                bb = quad_block(grp, t, zs, pr)
                for n in kinds:
                    for e in halves:
                        got(outs[n].at[rows_k(bb, e) if n < 2 else rows_q(zs, pr, e), :], rs1.at[zs * 2 + pr, n, e])

    def part(it, mask, kk):
        g2 = flip(grp, mask)
        r = rd(tile_of(base_tile(g2, kk), it // 2) * KT + g2[2] * UQ, UQ)
        return (ko_ref, vo_ref)[it % 2].at[r, :]

    def hop(it, r, mask):
        d = order(it)[r]
        ref = part(it, mask, t)
        m2 = mask | (1 << d)
        return rcopy(ref, ref, ss2.at[it, m2], rs2.at[it, m2], chip(flip(grp, 1 << d), head), t)

    def over(it, mask):
        ref = part(it, mask, t)
        return rcopy(ref, ref, ss3.at[it, mask], rs3.at[it, mask], c, 1 - t)

    def fresh(it, r):
        return [m | (1 << order(it)[r]) for m in below(order(it)[:r])]

    def arrived(it, r):
        for m in fresh(it, r):
            got(part(it, m, t), rs2.at[it, m])

    def relay(it, r):
        arrived(it, r)
        if r < 2:
            for m in below(order(it)[:r + 1]):
                hop(it, r + 1, m).start()
        for m in fresh(it, r):
            over(it, m).start()

    def ready(j):
        for it in (2 * j, 2 * j + 1):
            relay(it, 2)
        for it in (2 * j, 2 * j + 1):
            for m in range(8):
                got(part(it, m, 1 - t), rs3.at[it, m])

    swaps[0].wait_recv()
    each(kv_blocks)(project)
    first(send, (0, 1))
    each(kv_blocks + q_blocks, kv_blocks)(project)
    first(send, (2,))
    swaps[1].wait_recv()
    own_items = lambda e: range(4 * e, 4 * e + 4)
    for e in range(2):
        first_got((0, 1), (e,))
        for it in own_items(e):
            hop(it, 0, 0).start()
        for it in own_items(e):
            over(it, 0).start()
        each(q_blocks // 2 * (e + 1), q_blocks // 2 * e)(project_out)
        if e == 0:
            for it in own_items(0):
                relay(it, 0)
    for j in range(2):
        for it in (2 * j, 2 * j + 1):
            relay(it, 1)
        for it in (2 * j, 2 * j + 1):
            relay(it + 4, 0)
    first(send, (3,))
    first_got((2,))

    diff = ahead(grp[2])

    @each(4 * G)
    def _(idx):
        j, h = idx // G, idx % G
        qt_scr[idx] = qo_ref[rows_of(j), cols_of(h)].T

    def score(idx, g, e, masked):
        kt = g * NG + e
        s = mm(ko_ref[rd(kt * KT, KT), :], qt_scr[idx])
        if masked:
            s = jnp.where(diff <= (tile_of(i, idx // G) - kt) * KT, s, NINF)
        s_scr[e] = s
        return jnp.max(s.reshape(KT // 8, 8, UQ), axis=0)

    def top(ms):
        m = ms[0]
        for x in ms[1:]:
            m = jnp.maximum(m, x)
        return jnp.max(m, axis=0, keepdims=True) * C2

    def step(idx, g, nidx, ng, masked):
        mo = m_scr[line(idx), :]
        mn = jnp.maximum(mo, mx_scr[:])
        fade = jnp.exp2(mo - mn)
        l = l_scr[idx] * fade
        acc = None
        ms = []
        for e in range(NG):
            p = jnp.exp2(s_scr[e] * C2 - mn)
            l = l + jnp.sum(p.reshape(KT // 8, 8, UQ), axis=0)
            r = tm(vo_ref[rd((g * NG + e) * KT, KT), :], p.astype(BF))
            acc = r if acc is None else acc + r
            ms.append(score(nidx, ng, e, masked))
        ot_scr[idx] = ot_scr[idx] * fade + acc
        m_scr[line(idx), :] = mn
        l_scr[idx] = l
        mx_scr[:] = top(ms)

    ends = [tile_of(i, j) // NG for j in range(4)]
    per = S // TG // 4
    ready(0)
    for j in range(4):
        for h in range(G):
            ot_scr[j * G + h] = jnp.zeros((HD, UQ), F32)
            l_scr[j * G + h] = jnp.zeros((8, UQ), F32)
    m_scr[:] = jnp.full(m_scr.shape, jnp.finfo(F32).min)
    mx_scr[:] = top([score(0, 0, e, True) for e in range(NG)])

    @each(4)
    def _(a):
        @each(4 * G, a * G)
        def _(idx):
            j, h = idx // G, idx % G
            for jn in range(1, 4):
                @pl.when((a == jn - 1) & (idx == 4 * G - 1))
                def _():
                    ready(jn)

                if jn > 1:
                    @pl.when((a == 0) & (idx == G * jn - G))
                    def _():
                        relay(2 * jn, 1)
                        relay(2 * jn + 1, 1)
            end = ends[0] * (a == 0) + ends[1] * (a == 1) + ends[2] * (a == 2) + ends[3] * (a == 3)
            stop = jnp.where(j == a, end + 1, per * (a + 1))

            @each(stop, per * a)
            def _(g):
                more = g + 1 < stop
                wrap = idx == 4 * G - 1
                nidx = jnp.where(more, idx, jnp.where(wrap, jnp.minimum(a + 1, 3) * G, idx + 1))
                ng = jnp.where(more, g + 1, jnp.where(wrap, jnp.minimum(a + 1, 3), a) * per)
                masked = ng == tile_of(i, nidx // G) // NG

                @pl.when(masked)
                def _():
                    step(idx, g, nidx, ng, True)

                @pl.when(jnp.logical_not(masked))
                def _():
                    step(idx, g, nidx, ng, False)

            @pl.when(j == a)
            def _():
                lt = jnp.sum(l_scr[idx], axis=0, keepdims=True)
                l2_ref[line(idx), :] = m_scr[line(idx), :] + jnp.log2(lt)
                o_ref[rows_of(j), cols_of(h)] = (ot_scr[idx] / lt).T.astype(BF)

    first_got((3,))

    def finish():
        for it in range(8):
            for r in range(3):
                for m in below(order(it)[:r]):
                    hop(it, r, m).wait_send()
            for m in range(8):
                over(it, m).wait_send()
        first(sent, (0, 1, 2, 3))
        for cp in swaps:
            cp.wait_send()
    return finish


RES = (0, 4 * G, 8 * G, 8 * G + 4)


def owners(t):
    j = t >> 3
    odd, hi = j & 1, j >> 1
    h = (1 - 2 * odd) * t + odd * (15 + 16 * hi) - (1 - odd) * 16 * hi
    za, yk = h >> 2, h & 3
    k = yk >> 1
    return j, k, za, mirror(yk, k)


def backward(q_ref, do_ref, o_ref, l2_ref, k_ref, v_ref, res_ref,
             qt_scr, s_scr, dqt_scr, dkv, d_scr, dot_scr, dp_scr,
               rb0, rb1, rb2, rb3, fin, ssb, rsb, ss0, rs0, ss1, rs1, ss2, rs2, ss3, rs3):
    c, t_me, grp, head = me()
    zb, yb, xb = head
    hm = yb * 2 + xb
    i = base_tile(grp, t_me)
    NT = S // KT
    nbrs = [chip(flip(grp, 1 << d), head) for d in range(3)]

    def back(fn, j, n):
        zs = ((j + 1) // 2) % 2
        half = j // 2
        for e in range(2):
            par = turn(e, half)
            cc = quad_block(grp, t_me, zs, par)
            own = (cc == c) & (zb == t_me)
            wide = G * HD if n < 2 else HD
            if n < 2:
                src = o_ref.at[rd(j * UQ + e * PC, PC), :]
            else:
                src = fin.at[j, n - 2, e * PC:(e + 1) * PC, :]
            dst = res_ref.at[rd(half * PC, PC), pl.ds(pl.multiple_of(RES[n] * HD + hm * wide, HD), wide)]
            fn(src, dst, ssb.at[j, e, n], rsb.at[hm, half, n], cc, zb, own)

    def back_got(n):
        wide = G * HD if n < 2 else HD
        for hh in range(4):
            for half in range(2):
                got(res_ref.at[half * PC:(half + 1) * PC, RES[n] * HD + hh * wide:RES[n] * HD + (hh + 1) * wide], rsb.at[hh, half, n])

    def item(n, e):
        t = tile_at(n)
        j, k, za, ya = owners(t)
        hi = j >> 1
        half = (e + j) & 1
        same = [za == grp[0], ya == grp[1], half == grp[2]]
        if e:
            same = same[::-1]
            slots = [(j * 2 + 1) * 4 + za * 2 + ya, hi * 4 + za * 2 + ya, hi * 2 + za, hi]
        else:
            slots = [j * 8 + za * 2 + ya, j * 2 + ya, j, hi]
        there = [k == t_me]
        for d in range(3):
            there.append(there[d] & same[d])
        sends = [k != t_me] + [there[d] & jnp.logical_not(same[d]) for d in range(3)]
        return 2 * t + half, j, slots, there, sends

    def link(n, e, u, slots, r):
        if r == 0:
            return rcopy(dkv.at[u], rb0.at[slots[0]], ss0.at[slots[0]], rs0.at[slots[0]], c, 1 - t_me)
        rb, ss, rs = ((rb1, ss1, rs1), (rb2, ss2, rs2), (rb3, ss3, rs3))[r - 1]
        return rcopy(rb0.at[slots[0]], rb.at[e, slots[r]], ss.at[e, slots[r]], rs.at[e, slots[r]], nbrs[3 - r if e else r - 1], t_me)

    def over(n):
        for e in range(2):
            u, _, slots, _, sends = item(n, e)

            @pl.when(sends[0])
            def _():
                link(n, e, u, slots, 0).start()

    def stage(n, r):
        for e in range(2):
            u, j, slots, there, sends = item(n, e)
            acc = rb0.at[slots[0]]

            @pl.when(there[r])
            def _():
                if r == 0:
                    got(acc, rs0.at[slots[0]])
                    acc[...] = acc[...] + dkv[u]
                else:
                    rb, rs = ((rb1, rs1), (rb2, rs2), (rb3, rs3))[r - 1]
                    new = rb.at[e, slots[r]]
                    got(new, rs.at[e, slots[r]])
                    if r < 3:
                        acc[...] = acc[...] + new[...]
                    else:
                        fin[j, 0] = ((acc[0] + new[0]) * TSC).T.astype(BF)
                        fin[j, 1] = (acc[1] + new[1]).T.astype(BF)
                        back(send, j, 2)
                        back(send, j, 3)
            if r < 3:
                @pl.when(sends[r + 1])
                def _():
                    link(n, e, u, slots, r + 1).start()

    def tile_at(n):
        n = jnp.minimum(n, NT - 1)
        b, a, w = n >> 3, (n >> 1) & 3, n & 1
        low = 4 * (b + 1 - 2 * (b & 1)) + a + 2 - 4 * (a >> 1)
        return (1 - w) * (31 - 4 * b - a) + w * low

    def sums(n):
        for r in range(4):
            m = n - LAGS[r]

            @pl.when((m >= 0) & (m < NT))
            def _():
                stage(m, r)

    for j in range(4):
        back(send, j, 0)

    diff = ahead(grp[2])

    @each(4 * G)
    def _(idx):
        j, h = idx // G, idx % G
        rows, cols = rows_of(j), cols_of(h)
        prod = do_ref[rows, cols].astype(F32) * o_ref[rows, cols].astype(F32)
        d_scr[line(idx), :] = jnp.sum(prod.T, axis=0, keepdims=True)
        dqt_scr[idx] = jnp.zeros((HD, UQ), F32)
        dot_scr[idx] = do_ref[rows, cols].T
    last = [tile_of(i, j) for j in range(4)]

    def keys(t):
        return rd(t * KT, KT)

    def dots(t, j, h):
        s_scr[h] = mm(k_ref[keys(t), :], qt_scr[j * G + h])
        dp_scr[h] = mm(v_ref[keys(t), :], dot_scr[j * G + h])

    def first(n):
        return tile_at(n + (last[3] < tile_at(n)).astype(jnp.int32))

    for h in range(G):
        dots(first(jnp.int32(0)), 3, h)

    @each(NT)
    def _(n):
        t = tile_at(n)
        krows = keys(t)
        units = 0
        for j in range(4):
            units = units + (last[j] >= t).astype(jnp.int32)
        dkv[pl.ds(2 * t, 2)] = jnp.zeros((2, 2, HD, UQ), F32)

        @each(units)
        def _(jj):
            j = 3 - jj
            wrap = jj + 1 == units
            tn = jnp.where(wrap, first(n + 1), t)
            jn = jnp.where(wrap, 3, j - 1)
            off = (tile_of(i, j) - t) * KT
            k = k_ref[krows, :]
            dv = None
            dk = None
            for h in range(G):
                idx = j * G + h
                s = jnp.where(diff <= off, s_scr[h] * C2, NINF)
                pb = jnp.exp2(s - l2_ref[line(idx), :]).astype(BF)
                ds = (pb.astype(F32) * (dp_scr[h] - d_scr[line(idx), :])).astype(BF)
                dots(tn, jn, h)
                r1 = mt(dot_scr[idx], pb)
                r2 = mt(qt_scr[idx], ds)
                dv = r1 if dv is None else dv + r1
                dk = r2 if dk is None else dk + r2
                dqt_scr[idx] += tm(k, ds)
            for e in range(2):
                dkv[2 * t + e, 0] += dk[:, e * UQ:(e + 1) * UQ]
                dkv[2 * t + e, 1] += dv[:, e * UQ:(e + 1) * UQ]
        over(n)
        sums(n)

    back_got(0)
    for j in range(4):
        back(sent, j, 0)

    @each(4 * G)
    def _(idx):
        j, h = idx // G, idx % G
        o_ref[rows_of(j), cols_of(h)] = (dqt_scr[idx] * TSC).T.astype(BF)
    for j in range(4):
        back(send, j, 1)

    @each(NT + LAGS[3], NT)
    def _(n):
        sums(n)

    @each(NT)
    def _(n):
        for e in range(2):
            u, _, slots, _, sends = item(n, e)
            for r in range(4):
                @pl.when(sends[r])
                def _():
                    link(n, e, u, slots, r).wait_send()
    for n in range(1, 4):
        back_got(n)
        for j in range(4):
            back(sent, j, n)


def attention_kernel(x_ref, dy_ref, wq, wk, wv, wo, res_ref, qo, doo, ko, vo, o, l2, qt, s_scr, acc, *scr):
    finish = forward(x_ref, dy_ref, wq, wk, wv, wo, qo, doo, ko, vo, o, l2, qt, s_scr, acc, *scr[:18])
    backward(qo, doo, o, l2, ko, vo, res_ref, qt, s_scr, acc, *scr[18:])
    finish()


def attention(x, dy, wq, wk, wv, wo):
    dma = pltpu.SemaphoreType.DMA
    vm = pltpu.VMEM
    both = lambda *m: [dma(m)] * 2
    n, d = x.shape
    wide = vm((4 * UQ, G * HD), BF)
    turned = vm((4 * G, HD, UQ), BF)
    shared = [wide, wide, vm((S, HD), BF), vm((S, HD), BF), wide, vm((4 * G, UQ), F32), turned, vm((NG, KT, UQ), F32), vm((4 * G, HD, UQ), F32)]
    fwd = [vm((2 * n, 2 * wk.shape[1] + wq.shape[1]), BF), vm((2 * n, wq.shape[1]), BF), vm((n, d), BF), vm((n, d), BF),
           vm((2, d, PB), BF), vm((2, PB, d), BF), vm((4 * G, UQ), F32), vm((4 * G, 8, UQ), F32), vm((1, UQ), F32), *both(2), dma((2, 2)),
           *both(4, 4, 2), *both(8, 8), *both(8, 8)]
    bwd = [vm((S // UQ, 2, HD, UQ), F32), vm((4 * G, UQ), F32), turned,
           vm((G, KT, UQ), F32), vm((32, 2, HD, UQ), F32), vm((2, 8, 2, HD, UQ), F32),
           vm((2, 4, 2, HD, UQ), F32), vm((2, 2, 2, HD, UQ), F32), vm((4, 2, UQ, HD), BF), *both(4, 2, 4),
           *both(32), *both(2, 8), *both(2, 4), *both(2, 2)]
    return pl.pallas_call(
        attention_kernel,
        out_shape=shape((2 * n, 2 * wq.shape[1] + 2 * wk.shape[1]), BF), in_specs=[VM] * 2 + [ANY] * 4, out_specs=VM,
        scratch_shapes=shared + fwd + bwd, compiler_params=params(65472, 2), name='attention')(x, dy, wq, wk, wv, wo)


NB = 512
DEEP = 4


def out_kernel(res_ref, wo, wq, wk, wv, y_own, y_in, dx_own, dx_in, bo, bq, bk, bv, away, lsem, ssem, rsem):
    c, t = lax.axis_index('cp'), lax.axis_index('tp')
    rows, width = y_own.shape
    blocks = width // NB

    def cols(b):
        return rd(b * NB, NB)

    def part(n, wide):
        return res_ref[:, RES[n] * HD:RES[n] * HD + wide]

    def loads(n, b, fn):
        s = b % DEEP
        if n == 0:
            fn(pltpu.make_async_copy(wo.at[:, cols(b)], bo.at[s], lsem.at[0, s]))
        else:
            for m, (w, buf) in enumerate(((wq, bq), (wk, bk), (wv, bv))):
                fn(pltpu.make_async_copy(w.at[cols(b), :], buf.at[s], lsem.at[1 + m, s]))

    def start(cp):
        cp.start()

    def wait(cp):
        cp.wait()

    for n in range(2):
        for b in range(DEEP):
            loads(n, b, start)
    bar = pltpu.get_barrier_semaphore()
    pl.semaphore_signal(bar, 1, device_id=dev(c, 1 - t), device_id_type=pl.DeviceIdType.MESH)
    pl.semaphore_wait(bar, 1)

    def swap(n, b):
        return rcopy(away.at[n, b], (y_in, dx_in)[n].at[:, cols(b)], ssem.at[n, b], rsem.at[n, b], c, 1 - t)

    def block(n, b):
        s = b % DEEP
        loads(n, b, wait)
        if n == 0:
            r = mm(part(0, bo.shape[1]), bo[s])
        else:
            r = mt(part(1, bq.shape[2]), bq[s]) + mt(part(2, bk.shape[2]), bk[s]) + mt(part(3, bv.shape[2]), bv[s])

        own = (y_own, dx_own)[n]

        @pl.when(t == 0)
        def _():
            own[:, cols(b)] = r[:rows]
            away[n, b] = r[rows:]

        @pl.when(t == 1)
        def _():
            own[:, cols(b)] = r[rows:]
            away[n, b] = r[:rows]
        swap(n, b).start()

        @pl.when(b + DEEP < blocks)
        def _():
            loads(n, b + DEEP, start)

    for n in range(2):
        @each(blocks)
        def _(b):
            block(n, b)

    @each(blocks)
    def _(b):
        swap(0, b).wait()
        swap(1, b).wait()


def outputs(res, wo, wq, wk, wv):
    n, width = res.shape[0] // 2, wo.shape[1]
    b = width // NB
    dma = pltpu.SemaphoreType.DMA
    vm = pltpu.VMEM
    f = pl.pallas_call(
        out_kernel, out_shape=(shape((n, width), F32),) * 4, in_specs=[VM] + [HB] * 4, out_specs=(VM,) * 4,
        scratch_shapes=[vm((DEEP, wo.shape[0], NB), BF), vm((DEEP, NB, wq.shape[1]), BF), vm((DEEP, NB, wk.shape[1]), BF),
                        vm((DEEP, NB, wv.shape[1]), BF), vm((2, b, n, NB), F32), dma((4, DEEP)), dma((2, b)), dma((2, b))],
        compiler_params=params(46080, 1), name='outputs')
    y_own, y_in, dx_own, dx_in = f(res, wo, wq, wk, wv)
    return (y_own + y_in).astype(BF), (dx_own + dx_in).astype(BF)


def solution(mesh):
    row_spec = P(('dp', 'cp', 'tp'), None)

    def local_step(x_blk, dy_blk, w_query, w_key, w_value, w_out):
        res = attention(x_blk, dy_blk, w_query, w_key, w_value, w_out)
        return outputs(res, w_out, w_query, w_key, w_value)

    return jax.shard_map(local_step, mesh=mesh, in_specs=(row_spec, row_spec, P(None, 'tp'), P(None, 'tp'), P(None, 'tp'), P('tp', None)), out_specs=(row_spec, row_spec), check_vma=False)
```

```python
import functools

import jax
import jax.numpy as jnp
from jax import lax
from jax.experimental import pallas as pl
from jax.experimental.pallas import tpu as pltpu
from jax.sharding import PartitionSpec as P

HD = 128
PC = HD
S = 16384
G = 3
KT = 512
NG = 4
TG = KT * NG
UQ = 256
LAGS = (3, 7, 11, 15)
TSC = HD ** -0.5
C2 = TSC * 1.4426950408889634
NINF = -float('inf')
BF = jnp.bfloat16
F32 = jnp.float32


def dg(a, b, ca, cb):
    return lax.dot_general(a, b, (((ca,), (cb,)), ((), ())), preferred_element_type=F32)


def each(n, first=0):
    def run(body):
        def step(m, _):
            body(m)
            return 0
        lax.fori_loop(first, n, step, 0)
    return run


def mm(a, b):
    return dg(a, b, 1, 0)


def mt(a, b):
    return dg(a, b, 1, 1)


def tm(a, b):
    return dg(a, b, 0, 0)


def mirror(v, h):
    return v + h * (3 - 2 * v)


def turn(v, e):
    return v + e * (1 - 2 * v)


def split(c):
    co = (c // 16, (c // 4) % 4, c % 4)
    return tuple(mirror(v, v // 2) for v in co), tuple(v // 2 for v in co)


def chip(grp, head):
    z, y, x = (mirror(g, h) for g, h in zip(grp, head))
    return z * 16 + y * 4 + x


def base_tile(grp, k):
    return grp[0] * 4 + mirror(grp[1], k)


def bits(n):
    return n >> 1, n & 1


def tile_of(i, j):
    hi, odd = bits(j)
    return hi * 16 + odd * 15 + i - 2 * odd * i


def ahead(xa):
    row = lax.broadcasted_iota(jnp.int32, (KT, UQ), 0)
    col = lax.broadcasted_iota(jnp.int32, (KT, UQ), 1)
    quarter = row // PC
    piece = jnp.where(quarter == 0, 0, jnp.where(quarter == 1, 3, quarter - 1))
    late = col // PC
    return (piece - mirror(xa, late)) * PC + row % PC - col % PC


def flip(grp, mask):
    return tuple(1 - g if (mask >> d) & 1 else g for d, g in enumerate(grp))


def quad_block(grp, k, zs, par):
    return chip(grp, (zs, (zs + k) % 2, par))


def dev(c, t):
    return {'tp': t, 'cp': c}


def me():
    c, t = lax.axis_index('cp'), lax.axis_index('tp')
    grp, head = split(c)
    return c, t, grp, head


def line(n):
    return pl.ds(n, 1)


def cuts(n):
    return [pl.ds(m, n // 4) for m in range(0, n, n // 4)]


def rd(start, n):
    return pl.ds(pl.multiple_of(start, n), n)


def greet(c, t, grp, head):
    bar = pltpu.get_barrier_semaphore()
    for hh in range(8):
        for k in range(2):
            cc = chip(grp, (hh // 4, (hh // 2) % 2, hh % 2))

            @pl.when((cc != c) | (t != k))
            def _():
                pl.semaphore_signal(bar, 1, device_id=dev(cc, k), device_id_type=pl.DeviceIdType.MESH)
    for d in range(3):
        pl.semaphore_signal(bar, 1, device_id=dev(chip(flip(grp, 1 << d), head), t), device_id_type=pl.DeviceIdType.MESH)
    pl.semaphore_wait(bar, 18)


def rcopy(src, dst, ssem, rsem, cc, k):
    return pltpu.make_async_remote_copy(src_ref=src, dst_ref=dst, send_sem=ssem, recv_sem=rsem, device_id=dev(cc, k), device_id_type=pl.DeviceIdType.MESH)


def send(src, dst, ssem, rsem, cc, k, own):
    @pl.when(own)
    def _():
        pltpu.make_async_copy(src, dst, rsem).start()

    @pl.when(jnp.logical_not(own))
    def _():
        rcopy(src, dst, ssem, rsem, cc, k).start()


def sent(src, dst, ssem, rsem, cc, k, own):
    @pl.when(jnp.logical_not(own))
    def _():
        rcopy(src, dst, ssem, rsem, cc, k).wait_send()


def got(dst, rsem):
    pltpu.make_async_copy(dst, dst, rsem).wait()


def order(it):
    return [(it + r) % 3 for r in range(3)]


def below(dims):
    masks = [0]
    for d in dims:
        masks += [m | (1 << d) for m in masks]
    return masks


VM = pl.BlockSpec(memory_space=pltpu.VMEM)
ANY = pl.BlockSpec(memory_space=pl.ANY)
HB = pl.BlockSpec(memory_space=pltpu.HBM)


def params(kib, cid):
    return pltpu.CompilerParams(vmem_limit_bytes=kib * 1024, collective_id=cid, has_side_effects=True)


def shape(s, d):
    return jax.ShapeDtypeStruct(s, d)


def rows_of(j):
    return rd(j * UQ, UQ)


def cols_of(h):
    return rd(h * HD, HD)


PB = UQ


def forward(x_ref, dy_ref, wq, wk, wv, wo, qo_ref, doo_ref, ko_ref, vo_ref, o_ref, l2_ref, qt_scr, s_scr, ot_scr,
            wa, wb, lsem, kvq, dout, xp, dyp, m_scr, l_scr, mx_scr, xss, xrs, ss1, rs1, ss2, rs2, ss3, rs3):
    c, t, grp, head = me()
    peer = 1 - t
    zb, yb, xb = head
    par = xb
    k = (zb + yb) % 2
    i = base_tile(grp, t)
    outs = (ko_ref, vo_ref, qo_ref, doo_ref)
    half = x_ref.shape[0]
    kv_blocks, q_blocks = 2 * wk.shape[1] // PB, wq.shape[1] // PB

    def load(b):
        for w, at, n in ((wk, 0, kv_blocks // 2), (wv, kv_blocks // 2, kv_blocks // 2), (wq, kv_blocks, q_blocks)):
            @pl.when((b >= at) & (b < at + n))
            def _():
                for rows in cuts(w.shape[0]):
                    pltpu.make_async_copy(w.at[rows, rd((b - at) * PB, PB)], wa.at[b & 1, rows, :], lsem.at[0, b & 1]).start()

    def load_out(b):
        for cols in cuts(wo.shape[1]):
            pltpu.make_async_copy(wo.at[rd(b * PB, PB), cols], wb.at[b & 1, :, cols], lsem.at[1, b & 1]).start()

    def put(ref, b, r):
        ref[rd(t * half, half), rd(b * PB, PB)] = r[:half].astype(BF)
        ref[rd(peer * half, half), rd(b * PB, PB)] = r[half:].astype(BF)

    def project(b):
        got(wa.at[b & 1], lsem.at[0, b & 1])
        put(kvq, b, mm(jnp.concatenate([x_ref[...], xp[...]], 0), wa[b & 1]))
        load(b + 2)

    def project_out(b):
        got(wb.at[b & 1], lsem.at[1, b & 1])
        put(dout, b, mt(jnp.concatenate([dy_ref[...], dyp[...]], 0), wb[b & 1]))

        @pl.when(b + 2 < q_blocks)
        def _():
            load_out(b + 2)

    for b in range(2):
        load(jnp.int32(b))
        load_out(b)
    greet(c, t, grp, head)
    swaps = [rcopy(src, dst, xss.at[n], xrs.at[n], c, peer) for n, (src, dst) in enumerate(((x_ref, xp), (dy_ref, dyp)))]
    for cp in swaps:
        cp.start()

    def rows_q(zs, pr, e):
        return rd(mirror(zs, e) * UQ + turn(pr, e) * PC, PC)

    def rows_k(bb, e):
        q, half = bb // 4, (bb % 4) // 2
        return rd((q + e * (31 - 2 * q)) * KT + grp[2] * UQ + turn(half, e) * PC, PC)

    def first(fn, kinds, halves=(0, 1)):
        for e in halves:
            for hh in range(4):
                cc = chip(grp, (t, hh // 2, hh % 2))
                own = (cc == c) & (k == t)
                for n in kinds:
                    wide = HD if n < 2 else G * HD
                    at = (0, kv_blocks // 2 * PB, kv_blocks * PB, 0)[n] + hh * wide
                    src = (kvq, kvq, kvq, dout)[n].at[e * PC:(e + 1) * PC, at:at + wide]
                    dst = outs[n].at[rows_k(c, e) if n < 2 else rows_q(zb, par, e), :]
                    fn(src, dst, ss1.at[hh, n, e], rs1.at[zb * 2 + par, n, e], cc, k, own)

    def first_got(kinds, halves=(0, 1)):
        for zs in range(2):
            for pr in range(2):
                bb = quad_block(grp, t, zs, pr)
                for n in kinds:
                    for e in halves:
                        got(outs[n].at[rows_k(bb, e) if n < 2 else rows_q(zs, pr, e), :], rs1.at[zs * 2 + pr, n, e])

    def part(it, mask, kk):
        g2 = flip(grp, mask)
        r = rd(tile_of(base_tile(g2, kk), it // 2) * KT + g2[2] * UQ, UQ)
        return (ko_ref, vo_ref)[it % 2].at[r, :]

    def pair(j):
        return 2 * j, 2 * j + 1

    def hop(it, r, mask):
        d = order(it)[r]
        ref = part(it, mask, t)
        m2 = mask | (1 << d)
        return rcopy(ref, ref, ss2.at[it, m2], rs2.at[it, m2], chip(flip(grp, 1 << d), head), t)

    def over(it, mask):
        ref = part(it, mask, t)
        return rcopy(ref, ref, ss3.at[it, mask], rs3.at[it, mask], c, peer)

    def fresh(it, r):
        return [m | (1 << order(it)[r]) for m in below(order(it)[:r])]

    def arrived(it, r):
        for m in fresh(it, r):
            got(part(it, m, t), rs2.at[it, m])

    def relay(it, r):
        arrived(it, r)
        if r < 2:
            for m in below(order(it)[:r + 1]):
                hop(it, r + 1, m).start()
        for m in fresh(it, r):
            over(it, m).start()

    def ready(j):
        for it in pair(j):
            relay(it, 2)
        for it in pair(j):
            for m in range(8):
                got(part(it, m, peer), rs3.at[it, m])

    swaps[0].wait_recv()
    each(kv_blocks)(project)
    first(send, (0, 1))
    each(kv_blocks + q_blocks, kv_blocks)(project)
    first(send, (2,))
    swaps[1].wait_recv()
    for e in range(2):
        first_got((0, 1), (e,))
        items = pair(2 * e) + pair(2 * e + 1)
        for it in items:
            hop(it, 0, 0).start()
        for it in items:
            over(it, 0).start()
        each(q_blocks // 2 * (e + 1), q_blocks // 2 * e)(project_out)
        if e == 0:
            for it in items:
                relay(it, 0)
    for j in range(2):
        for it in pair(j):
            relay(it, 1)
        for it in pair(j):
            relay(it + 4, 0)
    first(send, (3,))
    first_got((2,))

    diff = ahead(grp[2])

    @each(4 * G)
    def _(idx):
        j, h = idx // G, idx % G
        qt_scr[idx] = qo_ref[rows_of(j), cols_of(h)].T

    def score(idx, g, e, masked):
        kt = g * NG + e
        s = mm(ko_ref[rd(kt * KT, KT), :], qt_scr[idx])
        if masked:
            s = jnp.where(diff <= (tile_of(i, idx // G) - kt) * KT, s, NINF)
        s_scr[e] = s
        return jnp.max(s.reshape(KT // 8, 8, UQ), axis=0)

    def top(ms):
        m = ms[0]
        for x in ms[1:]:
            m = jnp.maximum(m, x)
        return jnp.max(m, axis=0, keepdims=True) * C2

    def step(idx, g, nidx, ng, masked):
        mo = m_scr[line(idx), :]
        mn = jnp.maximum(mo, mx_scr[:])
        fade = jnp.exp2(mo - mn)
        l = l_scr[idx] * fade
        acc = None
        ms = []
        for e in range(NG):
            p = jnp.exp2(s_scr[e] * C2 - mn)
            l = l + jnp.sum(p.reshape(KT // 8, 8, UQ), axis=0)
            r = tm(vo_ref[rd((g * NG + e) * KT, KT), :], p.astype(BF))
            acc = r if acc is None else acc + r
            ms.append(score(nidx, ng, e, masked))
        ot_scr[idx] = ot_scr[idx] * fade + acc
        m_scr[line(idx), :] = mn
        l_scr[idx] = l
        mx_scr[:] = top(ms)

    ends = [tile_of(i, j) // NG for j in range(4)]
    per = S // TG // 4
    ready(0)
    for j in range(4):
        for h in range(G):
            ot_scr[j * G + h] = jnp.zeros((HD, UQ), F32)
            l_scr[j * G + h] = jnp.zeros((8, UQ), F32)
    m_scr[:] = jnp.full(m_scr.shape, jnp.finfo(F32).min)
    mx_scr[:] = top([score(0, 0, e, True) for e in range(NG)])

    @each(4)
    def _(a):
        @each(4 * G, a * G)
        def _(idx):
            j, h = idx // G, idx % G
            for jn in range(1, 4):
                @pl.when((a == jn - 1) & (idx == 4 * G - 1))
                def _():
                    ready(jn)

                if jn > 1:
                    @pl.when((a == 0) & (idx == G * jn - G))
                    def _():
                        for it in pair(jn):
                            relay(it, 1)
            end = sum(x * (a == m) for m, x in enumerate(ends))
            stop = jnp.where(j == a, end + 1, per * (a + 1))

            @each(stop, per * a)
            def _(g):
                more = g + 1 < stop
                wrap = idx == 4 * G - 1
                nidx = jnp.where(more, idx, jnp.where(wrap, jnp.minimum(a + 1, 3) * G, idx + 1))
                ng = jnp.where(more, g + 1, jnp.where(wrap, jnp.minimum(a + 1, 3), a) * per)
                masked = ng == tile_of(i, nidx // G) // NG

                @pl.when(masked)
                def _():
                    step(idx, g, nidx, ng, True)

                @pl.when(jnp.logical_not(masked))
                def _():
                    step(idx, g, nidx, ng, False)

            @pl.when(j == a)
            def _():
                lt = jnp.sum(l_scr[idx], axis=0, keepdims=True)
                l2_ref[line(idx), :] = m_scr[line(idx), :] + jnp.log2(lt)
                o_ref[rows_of(j), cols_of(h)] = (ot_scr[idx] / lt).T.astype(BF)

    first_got((3,))

    def finish():
        for it in range(8):
            for r in range(3):
                for m in below(order(it)[:r]):
                    hop(it, r, m).wait_send()
            for m in range(8):
                over(it, m).wait_send()
        first(sent, (0, 1, 2, 3))
        for cp in swaps:
            cp.wait_send()
    return finish


RES = (0, 4 * G, 0, 4)


def owners(t):
    j = t >> 3
    hi, odd = bits(j)
    h = tile_of(t, j) - hi * (1 - odd) * 32
    za, yk = h >> 2, h & 3
    k = yk >> 1
    return j, k, za, mirror(yk, k)


def backward(q_ref, do_ref, o_ref, l2_ref, k_ref, v_ref, wq, wo, kvb_ref, y_ref, dx_ref,
             qt_scr, s_scr, dqt_scr, wa, wb, lsem, res, osem, dkv, d_scr, dot_scr, dp_scr,
               rb0, rb1, rb2, rb3, fin, ssb, rsb, ss0, rs0, ss1, rs1, ss2, rs2, ss3, rs3):
    c, t_me, grp, head = me()
    zb, yb, xb = head
    hm = yb * 2 + xb
    i = base_tile(grp, t_me)
    NT = S // KT
    nbrs = [chip(flip(grp, 1 << d), head) for d in range(3)]

    backs = (res, res, kvb_ref, kvb_ref)

    def back(fn, j, n):
        zs = ((j + 1) // 2) % 2
        half = j // 2
        for e in range(2):
            par = turn(e, half)
            cc = quad_block(grp, t_me, zs, par)
            own = (cc == c) & (zb == t_me)
            wide = G * HD if n < 2 else HD
            if n < 2:
                src = o_ref.at[rd(j * UQ + e * PC, PC), :]
            else:
                src = fin.at[j, n - 2, e * PC:(e + 1) * PC, :]
            dst = backs[n].at[rd(half * PC, PC), pl.ds(pl.multiple_of(RES[n] * HD + hm * wide, HD), wide)]
            fn(src, dst, ssb.at[j, e, n], rsb.at[hm, half, n], cc, zb, own)

    def back_got(n):
        wide = G * HD if n < 2 else HD
        for hh in range(4):
            for half in range(2):
                got(backs[n].at[half * PC:(half + 1) * PC, RES[n] * HD + hh * wide:RES[n] * HD + (hh + 1) * wide], rsb.at[hh, half, n])

    def whose(n):
        t = tile_at(n)
        return t, owners(t)

    def item(at, e):
        t, (j, k, za, ya) = at
        hi = j >> 1
        half = (e + j) & 1
        same = [za == grp[0], ya == grp[1], half == grp[2]]
        if e:
            same = same[::-1]
            slots = [(j * 2 + 1) * 4 + za * 2 + ya, hi * 4 + za * 2 + ya, hi * 2 + za, hi]
        else:
            slots = [j * 8 + za * 2 + ya, j * 2 + ya, j, hi]
        there = [k == t_me]
        for d in range(3):
            there.append(there[d] & same[d])
        sends = [k != t_me] + [there[d] & jnp.logical_not(same[d]) for d in range(3)]
        return 2 * t + half, j, slots, there, sends

    def link(e, u, slots, r):
        if r == 0:
            return rcopy(dkv.at[u], rb0.at[slots[0]], ss0.at[slots[0]], rs0.at[slots[0]], c, 1 - t_me)
        rb, ss, rs = ((rb1, ss1, rs1), (rb2, ss2, rs2), (rb3, ss3, rs3))[r - 1]
        return rcopy(rb0.at[slots[0]], rb.at[e, slots[r]], ss.at[e, slots[r]], rs.at[e, slots[r]], nbrs[3 - r if e else r - 1], t_me)

    def over(n):
        at = whose(n)
        for e in range(2):
            u, _, slots, _, sends = item(at, e)

            @pl.when(sends[0])
            def _():
                link(e, u, slots, 0).start()

    def stage(n, r):
        at = whose(n)
        for e in range(2):
            u, j, slots, there, sends = item(at, e)
            acc = rb0.at[slots[0]]

            @pl.when(there[r])
            def _():
                if r == 0:
                    got(acc, rs0.at[slots[0]])
                    acc[...] = acc[...] + dkv[u]
                else:
                    rb, rs = ((rb1, rs1), (rb2, rs2), (rb3, rs3))[r - 1]
                    new = rb.at[e, slots[r]]
                    got(new, rs.at[e, slots[r]])
                    if r < 3:
                        acc[...] = acc[...] + new[...]
                    else:
                        fin[j, 0] = ((acc[0] + new[0]) * TSC).T.astype(BF)
                        fin[j, 1] = (acc[1] + new[1]).T.astype(BF)
                        back(send, j, 2)
                        back(send, j, 3)
            if r < 3:
                @pl.when(sends[r + 1])
                def _():
                    link(e, u, slots, r + 1).start()

    inner, blocks = wo.shape[0], wo.shape[1] // UQ

    def weights(n, m):
        slot = m & 1
        if n:
            return wq.at[rd(m * UQ, UQ), :], wb.at[slot, :, :inner], lsem.at[n, slot]
        return wo.at[:, rd(m * UQ, UQ)], wa.at[slot, :inner, :], lsem.at[n, slot]

    def held(m):
        return s_scr.at[m & 3, :UQ, :]

    def stored(n, m):
        return pltpu.make_async_copy(held(m), (y_ref, dx_ref)[n].at[:, rd(m * UQ, UQ)], osem.at[m & 3])

    def product(n, m):
        got(*weights(n, m)[1:])

        @pl.when(m > 3)
        def _():
            stored(n, m - 4).wait()
        w = weights(n, m)[1]
        held(m)[:, :] = mt(res[:, inner:], w[:, :]) if n else mm(res[:, :inner], w[:, :])
        stored(n, m).start()

        @pl.when(m + 2 < blocks)
        def _():
            pltpu.make_async_copy(*weights(n, m + 2)).start()

    def products(n, m):
        product(n, 2 * m)
        product(n, 2 * m + 1)

    def settle(n):
        for m in range(blocks - 4, blocks):
            stored(n, m).wait()

    for n in range(2):
        for m in range(2):
            pltpu.make_async_copy(*weights(n, m)).start()

    def tile_at(n):
        n = jnp.minimum(n, NT - 1)
        b, a, w = n >> 3, (n >> 1) & 3, n & 1
        low = 4 * (b + 1 - 2 * (b & 1)) + a + 2 - 4 * (a >> 1)
        return (1 - w) * (31 - 4 * b - a) + w * low

    def sums(n):
        for r in range(4):
            m = n - LAGS[r]

            @pl.when((m >= 0) & (m < NT))
            def _():
                stage(m, r)

    for j in range(4):
        back(send, j, 0)

    diff = ahead(grp[2])

    @each(4 * G)
    def _(idx):
        j, h = idx // G, idx % G
        rows, cols = rows_of(j), cols_of(h)
        prod = do_ref[rows, cols].astype(F32) * o_ref[rows, cols].astype(F32)
        d_scr[line(idx), :] = jnp.sum(prod.T, axis=0, keepdims=True)
        dqt_scr[idx] = jnp.zeros((HD, UQ), F32)
        dot_scr[idx] = do_ref[rows, cols].T
    last = [tile_of(i, j) for j in range(4)]

    def keys(t):
        return rd(t * KT, KT)

    def dots(t, j, h):
        s_scr[h] = mm(k_ref[keys(t), :], qt_scr[j * G + h])
        dp_scr[h] = mm(v_ref[keys(t), :], dot_scr[j * G + h])

    def first(n):
        return tile_at(n + (last[3] < tile_at(n)).astype(jnp.int32))

    for h in range(G):
        dots(first(jnp.int32(0)), 3, h)

    @each(NT)
    def _(n):
        t = tile_at(n)
        krows = keys(t)
        units = 0
        for j in range(4):
            units = units + (last[j] >= t).astype(jnp.int32)
        dkv[pl.ds(2 * t, 2)] = jnp.zeros((2, 2, HD, UQ), F32)

        @each(units)
        def _(jj):
            j = 3 - jj
            wrap = jj + 1 == units
            tn = jnp.where(wrap, first(n + 1), t)
            jn = jnp.where(wrap, 3, j - 1)
            off = (tile_of(i, j) - t) * KT
            k = k_ref[krows, :]
            dv = None
            dk = None
            for h in range(G):
                idx = j * G + h
                s = jnp.where(diff <= off, s_scr[h] * C2, NINF)
                pb = jnp.exp2(s - l2_ref[line(idx), :]).astype(BF)
                ds = (pb.astype(F32) * (dp_scr[h] - d_scr[line(idx), :])).astype(BF)
                dots(tn, jn, h)
                r1 = mt(dot_scr[idx], pb)
                r2 = mt(qt_scr[idx], ds)
                dv = r1 if dv is None else dv + r1
                dk = r2 if dk is None else dk + r2
                dqt_scr[idx] += tm(k, ds)
            for e in range(2):
                dkv[2 * t + e, 0] += dk[:, e * UQ:(e + 1) * UQ]
                dkv[2 * t + e, 1] += dv[:, e * UQ:(e + 1) * UQ]
        over(n)
        sums(n)

    back_got(0)
    for j in range(4):
        back(sent, j, 0)

    @each(4 * G)
    def _(idx):
        j, h = idx // G, idx % G
        o_ref[rows_of(j), cols_of(h)] = (dqt_scr[idx] * TSC).T.astype(BF)
    for j in range(4):
        back(send, j, 1)

    late = NT + LAGS[3] - blocks // 2

    @each(NT + LAGS[3], NT)
    def _(n):
        sums(n)

        @pl.when(n < NT + blocks // 2)
        def _():
            products(0, n - NT)

        @pl.when(n == late)
        def _():
            settle(0)
            back_got(1)

        @pl.when(n >= late)
        def _():
            products(1, n - late)
    settle(1)

    @each(NT)
    def _(n):
        at = whose(n)
        for e in range(2):
            u, _, slots, _, sends = item(at, e)
            for r in range(4):
                @pl.when(sends[r])
                def _():
                    link(e, u, slots, r).wait_send()
    for n in (2, 3):
        back_got(n)
    for j in range(4):
        for n in (1, 2, 3):
            back(sent, j, n)


def attention_kernel(x_ref, dy_ref, wq, wk, wv, wo, kvb_ref, y_ref, dx_ref, qo, doo, ko, vo, o, l2, qt, s_scr, acc, wa, wb, lsem, *scr):
    finish = forward(x_ref, dy_ref, wq, wk, wv, wo, qo, doo, ko, vo, o, l2, qt, s_scr, acc, wa, wb, lsem, *scr[:15])
    backward(qo, doo, o, l2, ko, vo, wq, wo, kvb_ref, y_ref, dx_ref, qt, s_scr, acc, wa, wb, lsem, *scr[15:])
    finish()


def attention(x, dy, wq, wk, wv, wo):
    dma = pltpu.SemaphoreType.DMA
    vm = pltpu.VMEM
    both = lambda *m: [dma(m)] * 2
    n, d = x.shape
    wide = vm((4 * UQ, G * HD), BF)
    turned = vm((4 * G, HD, UQ), BF)
    shared = [wide, wide, vm((S, HD), BF), vm((S, HD), BF), wide, vm((4 * G, UQ), F32), turned, vm((NG, KT, UQ), F32), vm((4 * G, HD, UQ), F32),
              vm((2, d, PB), BF), vm((2, PB, d), BF), dma((2, 2))]
    fwd = [vm((2 * n, 2 * wk.shape[1] + wq.shape[1]), BF), vm((2 * n, wq.shape[1]), BF), vm((n, d), BF), vm((n, d), BF), vm((4 * G, UQ), F32), vm((4 * G, 8, UQ), F32), vm((1, UQ), F32), *both(2),
           *both(4, 4, 2), *both(8, 8), *both(8, 8)]
    bwd = [vm((2 * n, 2 * wq.shape[1]), BF), dma((4,)), vm((S // UQ, 2, HD, UQ), F32), vm((4 * G, UQ), F32), turned,
           vm((G, KT, UQ), F32), vm((32, 2, HD, UQ), F32), vm((2, 8, 2, HD, UQ), F32),
           vm((2, 4, 2, HD, UQ), F32), vm((2, 2, 2, HD, UQ), F32), vm((4, 2, UQ, HD), BF), *both(4, 2, 4),
           *both(32), *both(2, 8), *both(2, 4), *both(2, 2)]
    return pl.pallas_call(
        attention_kernel,
        out_shape=(shape((2 * n, 2 * wk.shape[1]), BF),) + (shape((2 * n, d), F32),) * 2, in_specs=[VM] * 2 + [ANY] * 4, out_specs=(VM, ANY, ANY),
        scratch_shapes=shared + fwd + bwd, compiler_params=params(65472, 2), name='attention')(x, dy, wq, wk, wv, wo)


NB = 512
DEEP = 4


def out_kernel(kv_ref, y_part, dx_part, wk, wv, y_own, y_in, dx_own, dx_in, bx, bk, bv, away, ysem, lsem, ssem, rsem):
    c, t = lax.axis_index('cp'), lax.axis_index('tp')
    rows, width = y_own.shape
    blocks, depth = width // NB, wk.shape[1]
    mine, other = rd(t * rows, rows), rd((1 - t) * rows, rows)

    def cols(b):
        return rd(b * NB, NB)

    def loads(b, fn):
        s = b & 3
        fn(wk.at[cols(b), :], bk.at[s], lsem.at[0, s])
        fn(wv.at[cols(b), :], bv.at[s], lsem.at[1, s])
        fn(dx_part.at[other, cols(b)], bx.at[s, :rows, :], lsem.at[2, s])
        fn(dx_part.at[mine, cols(b)], bx.at[s, rows:, :], lsem.at[3, s])

    def start(*cp):
        pltpu.make_async_copy(*cp).start()

    def wait(*cp):
        pltpu.make_async_copy(*cp).wait()

    def part(at):
        return jnp.concatenate([kv_ref[other, at], kv_ref[mine, at]], 0)

    start(y_part.at[mine, :], y_own, ysem)
    for b in range(DEEP):
        loads(b, start)
    bar = pltpu.get_barrier_semaphore()
    pl.semaphore_signal(bar, 1, device_id=dev(c, 1 - t), device_id_type=pl.DeviceIdType.MESH)
    pl.semaphore_wait(bar, 1)
    y_swap = rcopy(y_part.at[other, :], y_in, ssem.at[blocks], rsem.at[blocks], c, 1 - t)
    y_swap.start()

    def swap(b):
        return rcopy(away.at[b], dx_in.at[:, cols(b)], ssem.at[b], rsem.at[b], c, 1 - t)

    @each(blocks)
    def _(b):
        s = b & 3
        loads(b, wait)
        r = mt(part(pl.ds(0, depth)), bk[s]) + mt(part(pl.ds(depth, depth)), bv[s]) + bx[s]
        away[b] = r[:rows]
        dx_own[:, cols(b)] = r[rows:]
        swap(b).start()

        @pl.when(b + DEEP < blocks)
        def _():
            loads(b + DEEP, start)

    @each(blocks)
    def _(b):
        swap(b).wait()
    y_swap.wait()
    wait(y_part.at[mine, :], y_own, ysem)


def outputs(kv, y_part, dx_part, wk, wv):
    n, width = kv.shape[0] // 2, wk.shape[0]
    b = width // NB
    dma = pltpu.SemaphoreType.DMA
    vm = pltpu.VMEM
    f = pl.pallas_call(
        out_kernel, out_shape=(shape((n, width), F32),) * 4, in_specs=[VM] + [HB] * 4, out_specs=(VM,) * 4,
        scratch_shapes=[vm((DEEP, 2 * n, NB), F32), vm((DEEP, NB, wk.shape[1]), BF), vm((DEEP, NB, wk.shape[1]), BF),
                        vm((b, n, NB), F32), dma, dma((4, DEEP)), dma((b + 1,)), dma((b + 1,))],
        compiler_params=params(46080, 1), name='outputs')
    y_own, y_in, dx_own, dx_in = f(kv, y_part, dx_part, wk, wv)
    return (y_own + y_in).astype(BF), (dx_own + dx_in).astype(BF)


def solution(mesh):
    row_spec = P(('dp', 'cp', 'tp'), None)

    def local_step(x_blk, dy_blk, w_query, w_key, w_value, w_out):
        kv, y_part, dx_part = attention(x_blk, dy_blk, w_query, w_key, w_value, w_out)
        return outputs(kv, y_part, dx_part, w_key, w_value)

    return jax.shard_map(local_step, mesh=mesh, in_specs=(row_spec, row_spec, P(None, 'tp'), P(None, 'tp'), P(None, 'tp'), P('tp', None)), out_specs=(row_spec, row_spec), check_vma=False)
```

```python
import functools

import jax
import jax.numpy as jnp
from jax import lax
from jax.experimental import pallas as pl
from jax.experimental.pallas import tpu as pltpu
from jax.sharding import PartitionSpec as P

HD = 128
PC = HD
S = 16384
G = 3
KT = 512
NG = 4
TG = KT * NG
UQ = 256
LAGS = (3, 7, 11, 15)
TSC = HD ** -0.5
C2 = TSC * 1.4426950408889634
NINF = -float('inf')
BF = jnp.bfloat16
F32 = jnp.float32


def dg(a, b, ca, cb):
    return lax.dot_general(a, b, (((ca,), (cb,)), ((), ())), preferred_element_type=F32)


def each(n, first=0):
    def run(body):
        def step(m, _):
            body(m)
            return 0
        lax.fori_loop(first, n, step, 0)
    return run


def mm(a, b):
    return dg(a, b, 1, 0)


def mt(a, b):
    return dg(a, b, 1, 1)


def tm(a, b):
    return dg(a, b, 0, 0)


def mirror(v, h):
    return v + h * (3 - 2 * v)


def turn(v, e):
    return v + e * (1 - 2 * v)


def split(c):
    co = (c // 16, (c // 4) % 4, c % 4)
    return tuple(mirror(v, v // 2) for v in co), tuple(v // 2 for v in co)


def chip(grp, head):
    z, y, x = (mirror(g, h) for g, h in zip(grp, head))
    return z * 16 + y * 4 + x


def base_tile(grp, k):
    return grp[0] * 4 + mirror(grp[1], k)


def bits(n):
    return n >> 1, n & 1


def tile_of(i, j):
    hi, odd = bits(j)
    return hi * 16 + odd * 15 + i - 2 * odd * i


def ahead(xa):
    row = lax.broadcasted_iota(jnp.int32, (KT, UQ), 0)
    col = lax.broadcasted_iota(jnp.int32, (KT, UQ), 1)
    quarter = row // PC
    piece = jnp.where(quarter == 0, 0, jnp.where(quarter == 1, 3, quarter - 1))
    late = col // PC
    return (piece - mirror(xa, late)) * PC + row % PC - col % PC


def flip(grp, mask):
    return tuple(1 - g if (mask >> d) & 1 else g for d, g in enumerate(grp))


def quad_block(grp, k, zs, par):
    return chip(grp, (zs, (zs + k) % 2, par))


def dev(c, t):
    return {'tp': t, 'cp': c}


def me():
    c, t = lax.axis_index('cp'), lax.axis_index('tp')
    grp, head = split(c)
    return c, t, grp, head


def line(n):
    return pl.ds(n, 1)


def cuts(n):
    return [pl.ds(m, n // 4) for m in range(0, n, n // 4)]


def rd(start, n):
    return pl.ds(pl.multiple_of(start, n), n)


def greet(c, t, grp, head):
    bar = pltpu.get_barrier_semaphore()
    for hh in range(8):
        for k in range(2):
            cc = chip(grp, (hh // 4, (hh // 2) % 2, hh % 2))

            @pl.when((cc != c) | (t != k))
            def _():
                pl.semaphore_signal(bar, 1, device_id=dev(cc, k), device_id_type=pl.DeviceIdType.MESH)
    for d in range(3):
        pl.semaphore_signal(bar, 1, device_id=dev(chip(flip(grp, 1 << d), head), t), device_id_type=pl.DeviceIdType.MESH)
    pl.semaphore_wait(bar, 18)


def rcopy(src, dst, ssem, rsem, cc, k):
    return pltpu.make_async_remote_copy(src_ref=src, dst_ref=dst, send_sem=ssem, recv_sem=rsem, device_id=dev(cc, k), device_id_type=pl.DeviceIdType.MESH)


def send(src, dst, ssem, rsem, cc, k, own):
    @pl.when(own)
    def _():
        pltpu.make_async_copy(src, dst, rsem).start()

    @pl.when(jnp.logical_not(own))
    def _():
        rcopy(src, dst, ssem, rsem, cc, k).start()


def sent(src, dst, ssem, rsem, cc, k, own):
    @pl.when(jnp.logical_not(own))
    def _():
        rcopy(src, dst, ssem, rsem, cc, k).wait_send()


def got(dst, rsem):
    pltpu.make_async_copy(dst, dst, rsem).wait()


def order(it):
    return [(it + r) % 3 for r in range(3)]


def below(dims):
    masks = [0]
    for d in dims:
        masks += [m | (1 << d) for m in masks]
    return masks


VM = pl.BlockSpec(memory_space=pltpu.VMEM)
ANY = pl.BlockSpec(memory_space=pl.ANY)
HB = pl.BlockSpec(memory_space=pltpu.HBM)


def params(kib, cid):
    return pltpu.CompilerParams(vmem_limit_bytes=kib * 1024, collective_id=cid, has_side_effects=True)


def shape(s, d):
    return jax.ShapeDtypeStruct(s, d)


def rows_of(j):
    return rd(j * UQ, UQ)


def cols_of(h):
    return rd(h * HD, HD)


PB = UQ


def forward(x_ref, dy_ref, wq, wk, wv, wo, qo_ref, doo_ref, ko_ref, vo_ref, o_ref, l2_ref, qt_scr, s_scr, ot_scr,
            wa, wb, lsem, kvq, dout, xp, dyp, m_scr, l_scr, mx_scr, xss, xrs, ss1, rs1, ss2, rs2, ss3, rs3):
    c, t, grp, head = me()
    peer = 1 - t
    zb, yb, xb = head
    par = xb
    k = (zb + yb) % 2
    i = base_tile(grp, t)
    outs = (ko_ref, vo_ref, qo_ref, doo_ref)
    half = x_ref.shape[0]
    kv_blocks, q_blocks = 2 * wk.shape[1] // PB, wq.shape[1] // PB

    def load(b):
        for w, at, n in ((wk, 0, kv_blocks // 2), (wv, kv_blocks // 2, kv_blocks // 2), (wq, kv_blocks, q_blocks)):
            @pl.when((b >= at) & (b < at + n))
            def _():
                for rows in cuts(w.shape[0]):
                    pltpu.make_async_copy(w.at[rows, rd((b - at) * PB, PB)], wa.at[b & 1, rows, :], lsem.at[0, b & 1]).start()

    def load_out(b):
        for cols in cuts(wo.shape[1]):
            pltpu.make_async_copy(wo.at[rd(b * PB, PB), cols], wb.at[b & 1, :, cols], lsem.at[1, b & 1]).start()

    def put(ref, b, r):
        ref[rd(t * half, half), rd(b * PB, PB)] = r[:half].astype(BF)
        ref[rd(peer * half, half), rd(b * PB, PB)] = r[half:].astype(BF)

    def project(b):
        got(wa.at[b & 1], lsem.at[0, b & 1])
        put(kvq, b, mm(jnp.concatenate([x_ref[...], xp[...]], 0), wa[b & 1]))
        load(b + 2)

    def project_out(b):
        got(wb.at[b & 1], lsem.at[1, b & 1])
        put(dout, b, mt(jnp.concatenate([dy_ref[...], dyp[...]], 0), wb[b & 1]))

        @pl.when(b + 2 < q_blocks)
        def _():
            load_out(b + 2)

    for b in range(2):
        load(jnp.int32(b))
        load_out(b)
    greet(c, t, grp, head)
    swaps = [rcopy(src, dst, xss.at[n], xrs.at[n], c, peer) for n, (src, dst) in enumerate(((x_ref, xp), (dy_ref, dyp)))]
    for cp in swaps:
        cp.start()

    def rows_q(zs, pr, e):
        return rd(mirror(zs, e) * UQ + turn(pr, e) * PC, PC)

    def rows_k(bb, e):
        q, half = bb // 4, (bb % 4) // 2
        return rd((q + e * (31 - 2 * q)) * KT + grp[2] * UQ + turn(half, e) * PC, PC)

    def first(fn, kinds, halves=(0, 1)):
        for e in halves:
            for hh in range(4):
                cc = chip(grp, (t, hh // 2, hh % 2))
                own = (cc == c) & (k == t)
                for n in kinds:
                    wide = HD if n < 2 else G * HD
                    at = (0, kv_blocks // 2 * PB, kv_blocks * PB, 0)[n] + hh * wide
                    src = (kvq, kvq, kvq, dout)[n].at[e * PC:(e + 1) * PC, at:at + wide]
                    dst = outs[n].at[rows_k(c, e) if n < 2 else rows_q(zb, par, e), :]
                    fn(src, dst, ss1.at[hh, n, e], rs1.at[zb * 2 + par, n, e], cc, k, own)

    def first_got(kinds, halves=(0, 1)):
        for zs in range(2):
            for pr in range(2):
                bb = quad_block(grp, t, zs, pr)
                for n in kinds:
                    for e in halves:
                        got(outs[n].at[rows_k(bb, e) if n < 2 else rows_q(zs, pr, e), :], rs1.at[zs * 2 + pr, n, e])

    def part(it, mask, kk):
        g2 = flip(grp, mask)
        r = rd(tile_of(base_tile(g2, kk), it // 2) * KT + g2[2] * UQ, UQ)
        return (ko_ref, vo_ref)[it % 2].at[r, :]

    def pair(j):
        return 2 * j, 2 * j + 1

    def hop(it, r, mask):
        d = order(it)[r]
        ref = part(it, mask, t)
        m2 = mask | (1 << d)
        return rcopy(ref, ref, ss2.at[it, m2], rs2.at[it, m2], chip(flip(grp, 1 << d), head), t)

    def over(it, mask):
        ref = part(it, mask, t)
        return rcopy(ref, ref, ss3.at[it, mask], rs3.at[it, mask], c, peer)

    def fresh(it, r):
        return [m | (1 << order(it)[r]) for m in below(order(it)[:r])]

    def arrived(it, r):
        for m in fresh(it, r):
            got(part(it, m, t), rs2.at[it, m])

    def relay(it, r):
        arrived(it, r)
        if r < 2:
            for m in below(order(it)[:r + 1]):
                hop(it, r + 1, m).start()
        for m in fresh(it, r):
            over(it, m).start()

    def ready(j):
        for it in pair(j):
            relay(it, 2)
        for it in pair(j):
            for m in range(8):
                got(part(it, m, peer), rs3.at[it, m])

    swaps[0].wait_recv()
    each(kv_blocks)(project)
    first(send, (0, 1))
    each(kv_blocks + q_blocks, kv_blocks)(project)
    first(send, (2,))
    swaps[1].wait_recv()
    for e in range(2):
        first_got((0, 1), (e,))
        items = pair(2 * e) + pair(2 * e + 1)
        for it in items:
            hop(it, 0, 0).start()
        for it in items:
            over(it, 0).start()
        each(q_blocks // 2 * (e + 1), q_blocks // 2 * e)(project_out)
        if e == 0:
            for it in items:
                relay(it, 0)
    for j in range(2):
        for it in pair(j):
            relay(it, 1)
        for it in pair(j):
            relay(it + 4, 0)
    first(send, (3,))
    first_got((2,))

    diff = ahead(grp[2])

    @each(4 * G)
    def _(idx):
        j, h = idx // G, idx % G
        qt_scr[idx] = qo_ref[rows_of(j), cols_of(h)].T

    def score(idx, g, e, masked):
        kt = g * NG + e
        s = mm(ko_ref[rd(kt * KT, KT), :], qt_scr[idx])
        if masked:
            s = jnp.where(diff <= (tile_of(i, idx // G) - kt) * KT, s, NINF)
        s_scr[e] = s
        return jnp.max(s.reshape(KT // 8, 8, UQ), axis=0)

    def top(ms):
        m = ms[0]
        for x in ms[1:]:
            m = jnp.maximum(m, x)
        return jnp.max(m, axis=0, keepdims=True) * C2

    def step(idx, g, nidx, ng, masked):
        mo = m_scr[line(idx), :]
        mn = jnp.maximum(mo, mx_scr[:])
        fade = jnp.exp2(mo - mn)
        l = l_scr[idx] * fade
        acc = None
        ms = []
        for e in range(NG):
            p = jnp.exp2(s_scr[e] * C2 - mn)
            l = l + jnp.sum(p.reshape(KT // 8, 8, UQ), axis=0)
            r = tm(vo_ref[rd((g * NG + e) * KT, KT), :], p.astype(BF))
            acc = r if acc is None else acc + r
            ms.append(score(nidx, ng, e, masked))
        ot_scr[idx] = ot_scr[idx] * fade + acc
        m_scr[line(idx), :] = mn
        l_scr[idx] = l
        mx_scr[:] = top(ms)

    ends = [tile_of(i, j) // NG for j in range(4)]
    per = S // TG // 4
    ready(0)
    for j in range(4):
        for h in range(G):
            ot_scr[j * G + h] = jnp.zeros((HD, UQ), F32)
            l_scr[j * G + h] = jnp.zeros((8, UQ), F32)
    m_scr[:] = jnp.full(m_scr.shape, jnp.finfo(F32).min)
    mx_scr[:] = top([score(0, 0, e, True) for e in range(NG)])

    @each(4)
    def _(a):
        @each(4 * G, a * G)
        def _(idx):
            j, h = idx // G, idx % G
            for jn in range(1, 4):
                @pl.when((a == jn - 1) & (idx == 4 * G - 1))
                def _():
                    ready(jn)

                if jn > 1:
                    @pl.when((a == 0) & (idx == G * jn - G))
                    def _():
                        for it in pair(jn):
                            relay(it, 1)
            end = sum(x * (a == m) for m, x in enumerate(ends))
            stop = jnp.where(j == a, end + 1, per * (a + 1))

            @each(stop, per * a)
            def _(g):
                more = g + 1 < stop
                wrap = idx == 4 * G - 1
                nidx = jnp.where(more, idx, jnp.where(wrap, jnp.minimum(a + 1, 3) * G, idx + 1))
                ng = jnp.where(more, g + 1, jnp.where(wrap, jnp.minimum(a + 1, 3), a) * per)
                masked = ng == tile_of(i, nidx // G) // NG

                @pl.when(masked)
                def _():
                    step(idx, g, nidx, ng, True)

                @pl.when(jnp.logical_not(masked))
                def _():
                    step(idx, g, nidx, ng, False)

            @pl.when(j == a)
            def _():
                lt = jnp.sum(l_scr[idx], axis=0, keepdims=True)
                l2_ref[line(idx), :] = m_scr[line(idx), :] + jnp.log2(lt)
                o_ref[rows_of(j), cols_of(h)] = (ot_scr[idx] / lt).T.astype(BF)

    first_got((3,))

    def finish():
        for it in range(8):
            for r in range(3):
                for m in below(order(it)[:r]):
                    hop(it, r, m).wait_send()
            for m in range(8):
                over(it, m).wait_send()
        first(sent, (0, 1, 2, 3))
        for cp in swaps:
            cp.wait_send()
    return finish


RES = (0, 4 * G, 0, 4)


def owners(t):
    j = t >> 3
    hi, odd = bits(j)
    h = tile_of(t, j) - hi * (1 - odd) * 32
    za, yk = h >> 2, h & 3
    k = yk >> 1
    return j, k, za, mirror(yk, k)


def backward(q_ref, do_ref, o_ref, l2_ref, k_ref, v_ref, wq, wo, kvb_ref, y_ref, dx_ref,
             qt_scr, s_scr, dqt_scr, wa, wb, lsem, res, osem, dkv, d_scr, dot_scr, dp_scr,
               rb0, rb1, rb2, rb3, fin, ssb, rsb, ss0, rs0, ss1, rs1, ss2, rs2, ss3, rs3):
    c, t_me, grp, head = me()
    zb, yb, xb = head
    hm = yb * 2 + xb
    i = base_tile(grp, t_me)
    NT = S // KT
    nbrs = [chip(flip(grp, 1 << d), head) for d in range(3)]

    backs = (res, res, kvb_ref, kvb_ref)

    def back(fn, j, n):
        zs = ((j + 1) // 2) % 2
        half = j // 2
        for e in range(2):
            par = turn(e, half)
            cc = quad_block(grp, t_me, zs, par)
            own = (cc == c) & (zb == t_me)
            wide = G * HD if n < 2 else HD
            if n < 2:
                src = o_ref.at[rd(j * UQ + e * PC, PC), :]
            else:
                src = fin.at[j, n - 2, e * PC:(e + 1) * PC, :]
            dst = backs[n].at[rd(half * PC, PC), pl.ds(pl.multiple_of(RES[n] * HD + hm * wide, HD), wide)]
            fn(src, dst, ssb.at[j, e, n], rsb.at[hm, half, n], cc, zb, own)

    def back_got(n):
        wide = G * HD if n < 2 else HD
        for hh in range(4):
            for half in range(2):
                got(backs[n].at[half * PC:(half + 1) * PC, RES[n] * HD + hh * wide:RES[n] * HD + (hh + 1) * wide], rsb.at[hh, half, n])

    def whose(n):
        t = tile_at(n)
        return t, owners(t)

    def full(t):
        return t < NT - 4

    def item(at, e):
        t, (j, k, za, ya) = at
        hi = j >> 1
        half = (e + j) & 1
        same = [za == grp[0], ya == grp[1], half == grp[2]]
        if e:
            same = same[::-1]
            slots = [(j * 2 + 1) * 4 + za * 2 + ya, hi * 4 + za * 2 + ya, hi * 2 + za, hi]
        else:
            slots = [j * 8 + za * 2 + ya, j * 2 + ya, j, hi]
        there = [k == t_me]
        for d in range(3):
            there.append(there[d] & same[d])
        sends = [k != t_me] + [there[d] & jnp.logical_not(same[d]) for d in range(3)]
        if not e:
            sends[1] = sends[1] & full(t)
        return 2 * t + half, j, slots, there, sends

    def link(e, u, slots, r):
        if r == 0:
            return rcopy(dkv.at[u], rb0.at[slots[0]], ss0.at[slots[0]], rs0.at[slots[0]], c, 1 - t_me)
        rb, ss, rs = ((rb1, ss1, rs1), (rb2, ss2, rs2), (rb3, ss3, rs3))[r - 1]
        return rcopy(rb0.at[slots[0]], rb.at[e, slots[r]], ss.at[e, slots[r]], rs.at[e, slots[r]], nbrs[3 - r if e else r - 1], t_me)

    def over(n):
        at = whose(n)
        for e in range(2):
            u, _, slots, _, sends = item(at, e)

            @pl.when(sends[0])
            def _():
                link(e, u, slots, 0).start()

    def stage(n, r):
        at = whose(n)
        for e in range(2):
            u, j, slots, there, sends = item(at, e)
            acc = rb0.at[slots[0]]

            @pl.when(there[r] & full(at[0]) if r == 1 and not e else there[r])
            def _():
                if r == 0:
                    got(acc, rs0.at[slots[0]])
                    acc[...] = acc[...] + dkv[u]
                else:
                    rb, rs = ((rb1, rs1), (rb2, rs2), (rb3, rs3))[r - 1]
                    new = rb.at[e, slots[r]]
                    got(new, rs.at[e, slots[r]])
                    if r < 3:
                        acc[...] = acc[...] + new[...]
                    else:
                        fin[j, 0] = ((acc[0] + new[0]) * TSC).T.astype(BF)
                        fin[j, 1] = (acc[1] + new[1]).T.astype(BF)
                        back(send, j, 2)
                        back(send, j, 3)
            if r < 3:
                @pl.when(sends[r + 1])
                def _():
                    link(e, u, slots, r + 1).start()

    inner, blocks = wo.shape[0], wo.shape[1] // UQ

    def weights(n, m):
        slot = m & 1
        if n:
            return wq.at[rd(m * UQ, UQ), :], wb.at[slot, :, :inner], lsem.at[n, slot]
        return wo.at[:, rd(m * UQ, UQ)], wa.at[slot, :inner, :], lsem.at[n, slot]

    def held(m):
        return s_scr.at[m & 3, :UQ, :]

    def stored(n, m):
        return pltpu.make_async_copy(held(m), (y_ref, dx_ref)[n].at[:, rd(m * UQ, UQ)], osem.at[m & 3])

    def product(n, m):
        got(*weights(n, m)[1:])

        @pl.when(m > 3)
        def _():
            stored(n, m - 4).wait()
        w = weights(n, m)[1]
        held(m)[:, :] = mt(res[:, inner:], w[:, :]) if n else mm(res[:, :inner], w[:, :])
        stored(n, m).start()

        @pl.when(m + 2 < blocks)
        def _():
            pltpu.make_async_copy(*weights(n, m + 2)).start()

    def products(n, m):
        product(n, 2 * m)
        product(n, 2 * m + 1)

    def settle(n):
        for m in range(blocks - 4, blocks):
            stored(n, m).wait()

    for n in range(2):
        for m in range(2):
            pltpu.make_async_copy(*weights(n, m)).start()

    def tile_at(n):
        n = jnp.minimum(n, NT - 1)
        b, a, w = n >> 3, (n >> 1) & 3, n & 1
        low = 4 * (b + 1 - 2 * (b & 1)) + a + 2 - 4 * (a >> 1)
        return (1 - w) * (31 - 4 * b - a) + w * low

    def sums(n):
        for r in range(4):
            m = n - LAGS[r]

            @pl.when((m >= 0) & (m < NT))
            def _():
                stage(m, r)

    for j in range(4):
        back(send, j, 0)

    diff = ahead(grp[2])

    @each(4 * G)
    def _(idx):
        j, h = idx // G, idx % G
        rows, cols = rows_of(j), cols_of(h)
        prod = do_ref[rows, cols].astype(F32) * o_ref[rows, cols].astype(F32)
        d_scr[line(idx), :] = jnp.sum(prod.T, axis=0, keepdims=True)
        dqt_scr[idx] = jnp.zeros((HD, UQ), F32)
        dot_scr[idx] = do_ref[rows, cols].T
    last = [tile_of(i, j) for j in range(4)]

    def keys(t):
        return rd(t * KT, KT)

    def dots(t, j, h):
        s_scr[h] = mm(k_ref[keys(t), :], qt_scr[j * G + h])
        dp_scr[h] = mm(v_ref[keys(t), :], dot_scr[j * G + h])

    def first(n):
        return tile_at(n + (last[3] < tile_at(n)).astype(jnp.int32))

    for h in range(G):
        dots(first(jnp.int32(0)), 3, h)

    @each(NT)
    def _(n):
        t = tile_at(n)
        krows = keys(t)
        units = 0
        for j in range(4):
            units = units + (last[j] >= t).astype(jnp.int32)
        dkv[pl.ds(2 * t, 2)] = jnp.zeros((2, 2, HD, UQ), F32)

        @each(units)
        def _(jj):
            j = 3 - jj
            wrap = jj + 1 == units
            tn = jnp.where(wrap, first(n + 1), t)
            jn = jnp.where(wrap, 3, j - 1)
            off = (tile_of(i, j) - t) * KT
            k = k_ref[krows, :]
            dv = None
            dk = None
            for h in range(G):
                idx = j * G + h
                s = jnp.where(diff <= off, s_scr[h] * C2, NINF)
                pb = jnp.exp2(s - l2_ref[line(idx), :]).astype(BF)
                ds = (pb.astype(F32) * (dp_scr[h] - d_scr[line(idx), :])).astype(BF)
                dots(tn, jn, h)
                r1 = mt(dot_scr[idx], pb)
                r2 = mt(qt_scr[idx], ds)
                dv = r1 if dv is None else dv + r1
                dk = r2 if dk is None else dk + r2
                dqt_scr[idx] += tm(k, ds)
            for e in range(2):
                dkv[2 * t + e, 0] += dk[:, e * UQ:(e + 1) * UQ]
                dkv[2 * t + e, 1] += dv[:, e * UQ:(e + 1) * UQ]
        over(n)
        sums(n)

    back_got(0)
    for j in range(4):
        back(sent, j, 0)

    @each(4 * G)
    def _(idx):
        j, h = idx // G, idx % G
        o_ref[rows_of(j), cols_of(h)] = (dqt_scr[idx] * TSC).T.astype(BF)
    for j in range(4):
        back(send, j, 1)

    late = NT + LAGS[3] - blocks // 2

    @each(NT + LAGS[3], NT)
    def _(n):
        sums(n)

        @pl.when(n < NT + blocks // 2)
        def _():
            products(0, n - NT)

        @pl.when(n == late)
        def _():
            settle(0)
            back_got(1)

        @pl.when(n >= late)
        def _():
            products(1, n - late)
    settle(1)

    @each(NT)
    def _(n):
        at = whose(n)
        for e in range(2):
            u, _, slots, _, sends = item(at, e)
            for r in range(4):
                @pl.when(sends[r])
                def _():
                    link(e, u, slots, r).wait_send()
    for n in (2, 3):
        back_got(n)
    for j in range(4):
        for n in (1, 2, 3):
            back(sent, j, n)


def attention_kernel(x_ref, dy_ref, wq, wk, wv, wo, kvb_ref, y_ref, dx_ref, qo, doo, ko, vo, o, l2, qt, s_scr, acc, wa, wb, lsem, *scr):
    finish = forward(x_ref, dy_ref, wq, wk, wv, wo, qo, doo, ko, vo, o, l2, qt, s_scr, acc, wa, wb, lsem, *scr[:15])
    backward(qo, doo, o, l2, ko, vo, wq, wo, kvb_ref, y_ref, dx_ref, qt, s_scr, acc, wa, wb, lsem, *scr[15:])
    finish()


def attention(x, dy, wq, wk, wv, wo):
    dma = pltpu.SemaphoreType.DMA
    vm = pltpu.VMEM
    both = lambda *m: [dma(m)] * 2
    n, d = x.shape
    wide = vm((4 * UQ, G * HD), BF)
    turned = vm((4 * G, HD, UQ), BF)
    shared = [wide, wide, vm((S, HD), BF), vm((S, HD), BF), wide, vm((4 * G, UQ), F32), turned, vm((NG, KT, UQ), F32), vm((4 * G, HD, UQ), F32),
              vm((2, d, PB), BF), vm((2, PB, d), BF), dma((2, 2))]
    fwd = [vm((2 * n, 2 * wk.shape[1] + wq.shape[1]), BF), vm((2 * n, wq.shape[1]), BF), vm((n, d), BF), vm((n, d), BF), vm((4 * G, UQ), F32), vm((4 * G, 8, UQ), F32), vm((1, UQ), F32), *both(2),
           *both(4, 4, 2), *both(8, 8), *both(8, 8)]
    bwd = [vm((2 * n, 2 * wq.shape[1]), BF), dma((4,)), vm((S // UQ, 2, HD, UQ), F32), vm((4 * G, UQ), F32), turned,
           vm((G, KT, UQ), F32), vm((32, 2, HD, UQ), F32), vm((2, 8, 2, HD, UQ), F32),
           vm((2, 4, 2, HD, UQ), F32), vm((2, 2, 2, HD, UQ), F32), vm((4, 2, UQ, HD), BF), *both(4, 2, 4),
           *both(32), *both(2, 8), *both(2, 4), *both(2, 2)]
    return pl.pallas_call(
        attention_kernel,
        out_shape=(shape((2 * n, 2 * wk.shape[1]), BF),) + (shape((2 * n, d), F32),) * 2, in_specs=[VM] * 2 + [ANY] * 4, out_specs=(VM, ANY, ANY),
        scratch_shapes=shared + fwd + bwd, compiler_params=params(65472, 2), name='attention')(x, dy, wq, wk, wv, wo)


NB = 512
DEEP = 4


def out_kernel(kv_ref, y_part, dx_part, wk, wv, y_own, y_in, dx_own, dx_in, bx, bk, bv, away, ysem, lsem, ssem, rsem):
    c, t = lax.axis_index('cp'), lax.axis_index('tp')
    rows, width = y_own.shape
    blocks, depth = width // NB, wk.shape[1]
    mine, other = rd(t * rows, rows), rd((1 - t) * rows, rows)

    def cols(b):
        return rd(b * NB, NB)

    def loads(b, fn):
        s = b & 3
        fn(wk.at[cols(b), :], bk.at[s], lsem.at[0, s])
        fn(wv.at[cols(b), :], bv.at[s], lsem.at[1, s])
        fn(dx_part.at[other, cols(b)], bx.at[s, :rows, :], lsem.at[2, s])
        fn(dx_part.at[mine, cols(b)], bx.at[s, rows:, :], lsem.at[3, s])

    def start(*cp):
        pltpu.make_async_copy(*cp).start()

    def wait(*cp):
        pltpu.make_async_copy(*cp).wait()

    def part(at):
        return jnp.concatenate([kv_ref[other, at], kv_ref[mine, at]], 0)

    start(y_part.at[mine, :], y_own, ysem)
    for b in range(DEEP):
        loads(b, start)
    bar = pltpu.get_barrier_semaphore()
    pl.semaphore_signal(bar, 1, device_id=dev(c, 1 - t), device_id_type=pl.DeviceIdType.MESH)
    pl.semaphore_wait(bar, 1)
    y_swap = rcopy(y_part.at[other, :], y_in, ssem.at[blocks], rsem.at[blocks], c, 1 - t)
    y_swap.start()

    def swap(b):
        return rcopy(away.at[b], dx_in.at[:, cols(b)], ssem.at[b], rsem.at[b], c, 1 - t)

    @each(blocks)
    def _(b):
        s = b & 3
        loads(b, wait)
        r = mt(part(pl.ds(0, depth)), bk[s]) + mt(part(pl.ds(depth, depth)), bv[s]) + bx[s]
        away[b] = r[:rows]
        dx_own[:, cols(b)] = r[rows:]
        swap(b).start()

        @pl.when(b + DEEP < blocks)
        def _():
            loads(b + DEEP, start)

    @each(blocks)
    def _(b):
        swap(b).wait()
    y_swap.wait()
    wait(y_part.at[mine, :], y_own, ysem)


def outputs(kv, y_part, dx_part, wk, wv):
    n, width = kv.shape[0] // 2, wk.shape[0]
    b = width // NB
    dma = pltpu.SemaphoreType.DMA
    vm = pltpu.VMEM
    f = pl.pallas_call(
        out_kernel, out_shape=(shape((n, width), F32),) * 4, in_specs=[VM] + [HB] * 4, out_specs=(VM,) * 4,
        scratch_shapes=[vm((DEEP, 2 * n, NB), F32), vm((DEEP, NB, wk.shape[1]), BF), vm((DEEP, NB, wk.shape[1]), BF),
                        vm((b, n, NB), F32), dma, dma((4, DEEP)), dma((b + 1,)), dma((b + 1,))],
        compiler_params=params(46080, 1), name='outputs')
    y_own, y_in, dx_own, dx_in = f(kv, y_part, dx_part, wk, wv)
    return (y_own + y_in).astype(BF), (dx_own + dx_in).astype(BF)


def solution(mesh):
    row_spec = P(('dp', 'cp', 'tp'), None)

    def local_step(x_blk, dy_blk, w_query, w_key, w_value, w_out):
        kv, y_part, dx_part = attention(x_blk, dy_blk, w_query, w_key, w_value, w_out)
        return outputs(kv, y_part, dx_part, w_key, w_value)

    return jax.shard_map(local_step, mesh=mesh, in_specs=(row_spec, row_spec, P(None, 'tp'), P(None, 'tp'), P(None, 'tp'), P('tp', None)), out_specs=(row_spec, row_spec), check_vma=False)
```
